256 devices in a mesh: py: 8 (over y, core), pz: 32 (over x, z).
Axes of the slice: x: 4, y: 4, z: 8, core: 2. Of those that a mesh axis runs over, the one named last changes fastest.
Arguments:
- wavefunctions: float32 [2, 8, 128, 128, 128], P(None, None, 'pz', 'py'), may hold values from -6 to 6
- potential: float32 [128, 128, 128], P('pz', 'py'), may hold values from -4 to 4
- cutoff_sq: int32 [1], replicated, may hold values from 2304 to 4096
- locked_mask: int32 [8], replicated, may hold values 0 or 1
Outputs:
- applied: float32 [2, 8, 128, 128, 128], P(None, None, 'pz', 'py')
- rayleigh: float32 [8], replicated
- residual_norm: float32 [8], replicated
The draws below stay inside these ranges and needn't reach their ends.
All inputs are finite; a program needn't handle non-finite values.
Results may differ from the reference program's by a relative error of at most 0.00005.
Values sent between devices are 32-bit elements; how exact they have to be, the bound alone decides.
A program may use at most 64 MiB of HBM per device.

```python
import math
import jax
import jax.numpy as jnp
from jax import lax

GRID = 128
NB = 8


def place_ends(entries, own_key, least, largest):
    extent = entries.shape
    place = [jax.random.randint(jax.random.fold_in(own_key, axis), (), 0, extent[axis]) for axis in range(len(extent))]
    entries = entries.at[tuple(place)].set(least)
    longest = extent.index(max(extent))
    place[longest] = (place[longest] + 1) % extent[longest]
    return entries.at[tuple(place)].set(largest)


def steps_of(stream_key, dims, pieces, smallest, top_value):
    def one(dim, parts):
        draws = jax.random.uniform(jax.random.fold_in(jax.random.fold_in(stream_key, 6), dim), (parts,), jnp.float32, smallest / len(pieces), top_value / len(pieces))
        return jnp.repeat(jnp.exp(draws), dims[dim] // parts).reshape((-1,) + (1,) * (len(dims) - dim - 1))

    level = one(*pieces[0])
    for cut in pieces[1:]:
        level = level * one(*cut)
    return level


def centred(rng, extent, scale, limit, shards=(), held_as=jnp.bfloat16):
    result = jax.random.normal(rng, extent, jnp.float32) * scale
    if len(shards) > 0:
        result = steps_of(rng, extent, shards, -0.22, 0.18) * result
    return jnp.clip(result, min=-limit, max=limit).astype(held_as)


def setup_inputs(seed: int = 0) -> dict:
    keys = jax.random.split(jax.random.key(seed), 5)
    return {
        "wavefunctions": centred(keys[0], (2, NB, GRID, GRID, GRID), 1.0, 6.0, ((2, 32), (3, 8)), jnp.float32),
        "potential": centred(keys[1], (GRID, GRID, GRID), 1.0, 4.0, ((0, 32), (1, 8)), jnp.float32),
        "cutoff_sq": jax.random.randint(keys[2], (1,), GRID * GRID * 9 // 64, GRID * GRID // 4 + 1).astype(jnp.int32),
        "locked_mask": place_ends((jax.random.randint(keys[3], (NB,), 0, 4) < 1).astype(jnp.int32), jax.random.fold_in(keys[3], 1), 0, 1),
    }


def reference(wavefunctions, potential, cutoff_sq, locked_mask):
    freq = jnp.arange(GRID, dtype=jnp.int32)
    signed = jnp.where(freq < GRID // 2, freq, freq - GRID)
    square = signed * signed
    total = square[:, None, None] + square[None, :, None] + square[None, None, :]
    keep = (total <= cutoff_sq[0]).astype(jnp.float32)
    kinetic = 0.5 * (math.pi / GRID) ** 2 * total.astype(jnp.float32) * keep

    def one_band(pair):
        real_part, imag_part = pair
        field = real_part + 1j * imag_part
        spectrum = jnp.fft.fftn(field)
        back = jnp.fft.ifftn(spectrum * kinetic)
        return (jnp.real(back) + potential * real_part, jnp.imag(back) + potential * imag_part)
    applied_real, applied_imag = lax.map(one_band, (wavefunctions[0], wavefunctions[1]))
    applied = jnp.stack([applied_real, applied_imag])
    norm_sq = lax.optimization_barrier(jnp.sum(wavefunctions * wavefunctions, axis=(0, 2, 3, 4)))
    correlation = lax.optimization_barrier(jnp.sum(wavefunctions * applied, axis=(0, 2, 3, 4)))
    rayleigh = correlation / norm_sq
    residual = applied - rayleigh[None, :, None, None, None] * wavefunctions
    residual_sq = lax.optimization_barrier(jnp.sum(residual * residual, axis=(0, 2, 3, 4)))
    residual_norm = jnp.sqrt(residual_sq / norm_sq) * (1.0 - locked_mask.astype(jnp.float32))
    return (applied, rayleigh, residual_norm)
```

```python
import functools
import math

import jax
import jax.numpy as jnp
import numpy as np
from jax import lax
from jax.experimental import pallas as pl
from jax.experimental.pallas import tpu as pltpu
from jax.sharding import PartitionSpec as P

N = 128
NB = 8
NY = 8
NZ = 32
ZL = N // NZ
YL = N // NY
BLK = ZL * (N // NZ)
MESH = pl.DeviceIdType.MESH
F32 = jnp.float32
BF16 = jnp.bfloat16


def basis():
    n = np.arange(N)
    rows = []
    for m in range(N):
        k = (m + 1) // 2
        angle = 2.0 * np.pi * ((k * n) % N) / N
        row = np.cos(angle) if (m % 2 == 1 or m == 0) else np.sin(angle)
        scale = 1.0 / N if k in (0, N // 2) else 2.0 / N
        rows.append(np.sqrt(scale) * row)
    return np.stack(rows)


def high_low(table):
    high = table.astype(BF16)
    low = (table - high.astype(np.float64)).astype(BF16)
    return high, low


def tables():
    f = basis()
    fh, fl = high_low(f)
    right_fwd = np.block([[fh.T, fl.T], [fh.T, fl.T]])
    right_inv = np.block([[fh, fl], [fh, fl]])
    left_fwd = np.block([[fh, fh], [fl, fl]])
    left_inv = np.block([[fh.T, fh.T], [fl.T, fl.T]])
    d = np.zeros((2, N, NZ, 2, ZL))
    for i in range(2):
        d[i, :, :, i, :] = f.reshape(N, NZ, ZL)
    d = d.reshape(2 * N, 2 * N)
    z_fwd = np.concatenate(high_low(d), axis=0)
    z_inv = np.concatenate(high_low(d.T), axis=0)
    return [right_fwd, right_inv, left_fwd, left_inv, z_fwd, z_inv]


def split(x):
    high = x.astype(BF16)
    low = (x - high.astype(F32)).astype(BF16)
    return high, low


def dot(a, b):
    return jnp.dot(a, b, preferred_element_type=F32)


def times_right(x, table):
    high, low = split(x)
    both = dot(jnp.concatenate([high, low], axis=1), table)
    return both[:, :N] + both[:, N:]


def times_left(table, x):
    high, low = split(x)
    both = dot(table, jnp.concatenate([high, low], axis=0))
    return both[:N] + both[N:]


def times_z(table, x):
    high, low = split(x)
    both = dot(table, high)
    return both[: 2 * N] + both[2 * N :] + dot(table[: 2 * N], low)


def kernel(
    u_hbm, v_hbm, cutoff, locked, rf_hbm, ri_hbm, lf_hbm, li_hbm, zf_hbm, zi_hbm,
    out, ray_ref, res_ref,
    u_in, v_in, rf, ri, lf, li, zf, zi,
    planes, pot, sent, got, back, ret, app, kin, row1, row2, tot1, tot2,
    in_sem, y_send, y_recv, z_send, z_recv, b_send, b_recv, o_send, o_recv, o_own, r_send, r_recv,
):
    my = lax.axis_index("py")
    mz = lax.axis_index("pz")

    def y_peer(k):
        return lax.rem(my + k, NY)

    def z_peer(k):
        x = lax.rem(mz // 8 + k // 8, 4)
        z = lax.rem(mz + k, 8)
        return x * 8 + z

    loads = [(u_hbm, u_in), (v_hbm, v_in), (rf_hbm, rf), (lf_hbm, lf), (zf_hbm, zf), (zi_hbm, zi), (li_hbm, li), (ri_hbm, ri)]
    loads = [pltpu.make_async_copy(a, b, in_sem.at[i]) for i, (a, b) in enumerate(loads)]
    for copy in loads:
        copy.start()

    barrier = pltpu.get_barrier_semaphore()

    @pl.loop(1, NZ)
    def _(k):
        pl.semaphore_signal(barrier, inc=1, device_id=(my, z_peer(k)), device_id_type=MESH)

    @pl.loop(1, NY)
    def _(k):
        pl.semaphore_signal(barrier, inc=1, device_id=(y_peer(k), mz), device_id_type=MESH)

    for h in range(2):
        r = lax.broadcasted_iota(jnp.int32, (2 * N, N), 0)
        c = lax.broadcasted_iota(jnp.int32, (2 * N, N), 1)
        ky = (mz * (N // NZ) + 2 * h + r // N + 1) // 2
        kz = (r % N + 1) // 2
        kx = (c + 1) // 2
        s = ky * ky + kz * kz + kx * kx
        kin[:, h * N : (h + 1) * N] = jnp.where(
            s <= cutoff[0], 0.5 * (math.pi / N) ** 2 * s.astype(F32), 0.0
        )

    for copy in loads:
        copy.wait()
    pl.semaphore_wait(barrier, NZ - 1 + NY - 1)

    def drain(ref, sem):
        pltpu.make_async_copy(ref, ref, sem).wait()

    mine = pl.ds(pl.multiple_of(my * YL, YL), YL)
    for part in range(2):
        @pl.loop(1, NY)
        def _(k, part=part):
            j = y_peer(k)
            pltpu.make_async_remote_copy(
                u_in.at[part, j], planes.at[part, :, mine, :], y_send.at[part], y_recv.at[part],
                device_id=(j, mz), device_id_type=MESH,
            ).start()
        planes[part, :, mine, :] = u_in[part, my]

    @pl.loop(1, NY)
    def _(k):
        j = y_peer(k)
        pltpu.make_async_remote_copy(
            v_in, pot.at[:, mine, :], y_send.at[2], y_recv.at[2],
            device_id=(j, mz), device_id_type=MESH,
        ).start()
    pot[:, mine, :] = v_in[...]

    others = pl.ds(0, (NY - 1) * YL)
    rows_mine = pl.ds(pl.multiple_of(mz * BLK, BLK), BLK)
    z_others = pl.ds(0, (NZ - 1) * BLK)

    for part in range(2):
        drain(planes.at[part, :, others, :], y_recv.at[part])
        x = times_right(planes[part].reshape(ZL * N, N), rf[...])
        x = jnp.concatenate([x[z * N : (z + 1) * N] for z in range(ZL)], axis=1)
        x = times_left(lf[...], x)
        for z in range(ZL):
            sent[part, pl.ds(z, N, stride=ZL), :] = x[:, z * N : (z + 1) * N]

        @pl.loop(1, NZ)
        def _(k, part=part):
            d = z_peer(k)
            pltpu.make_async_remote_copy(
                sent.at[part, pl.ds(pl.multiple_of(d * BLK, BLK), BLK), :], got.at[part, rows_mine, :],
                z_send.at[part], z_recv.at[part],
                device_id=(my, d), device_id_type=MESH,
            ).start()
        got[part, rows_mine, :] = sent[part, rows_mine, :]

    for part in range(2):
        drain(got.at[part, z_others, :], z_recv.at[part])
        g = got[part].reshape(NZ, 2, 8, N)
        x = jnp.concatenate([g[:, h].reshape(2 * N, N) for h in range(2)], axis=1)
        x = times_z(zf[...], x) * kin[...]
        x = times_z(zi[...], x)
        x = jnp.stack([x[:, h * N : (h + 1) * N].reshape(NZ, 8, N) for h in range(2)], axis=1)
        back[part] = x.reshape(NZ * BLK, N)

        @pl.loop(1, NZ)
        def _(k, part=part):
            d = z_peer(k)
            pltpu.make_async_remote_copy(
                back.at[part, pl.ds(pl.multiple_of(d * BLK, BLK), BLK), :], ret.at[part, rows_mine, :],
                b_send.at[part], b_recv.at[part],
                device_id=(my, d), device_id_type=MESH,
            ).start()
        ret[part, rows_mine, :] = back[part, rows_mine, :]

    drain(pot.at[:, others, :], y_recv.at[2])
    norm = corr = square = None
    for part in range(2):
        drain(ret.at[part, z_others, :], b_recv.at[part])
        x = jnp.concatenate([ret[part, pl.ds(z, N, stride=ZL), :] for z in range(ZL)], axis=1)
        x = times_left(li[...], x)
        x = jnp.concatenate([x[:, z * N : (z + 1) * N] for z in range(ZL)], axis=0)
        x = times_right(x, ri[...])
        field = planes[part].reshape(ZL * N, N)
        x = x + pot[...].reshape(ZL * N, N) * field
        app[part] = x.reshape(ZL, N, N)

        @pl.loop(1, NY)
        def _(k, part=part):
            j = y_peer(k)
            pltpu.make_async_remote_copy(
                app.at[part, :, pl.ds(pl.multiple_of(j * YL, YL), YL), :], out.at[part, my],
                o_send.at[part], o_recv.at[part],
                device_id=(j, mz), device_id_type=MESH,
            ).start()
        pltpu.make_async_copy(app.at[part, :, mine, :], out.at[part, my], o_own.at[part]).start()
        sums = [jnp.sum(a.reshape(-1, 8, N), axis=0) for a in (field * field, field * x, x * x)]
        if part == 0:
            norm, corr, square = sums
        else:
            norm, corr, square = norm + sums[0], corr + sums[1], square + sums[2]

    lane = lax.broadcasted_iota(jnp.int32, (1, N), 1)
    row = jnp.zeros((1, N), F32)
    for i, value in enumerate((norm, corr, square)):
        row = jnp.where(lane == 16 * i + my, jnp.sum(value), row)
    row1[...] = row
    tot1[mz] = row

    @pl.loop(1, NZ)
    def _(k):
        d = z_peer(k)
        pltpu.make_async_remote_copy(
            row1, tot1.at[mz], r_send.at[0], r_recv.at[0], device_id=(my, d), device_id_type=MESH
        ).start()

    drain(tot1.at[pl.ds(0, NZ - 1)], r_recv.at[0])
    row = jnp.sum(tot1[...], axis=0)
    row2[...] = row
    tot2[my] = row

    @pl.loop(1, NY)
    def _(k):
        j = y_peer(k)
        pltpu.make_async_remote_copy(
            row2, tot2.at[my], r_send.at[1], r_recv.at[1], device_id=(j, mz), device_id_type=MESH
        ).start()

    drain(tot2.at[pl.ds(0, NY - 1)], r_recv.at[1])
    row = jnp.sum(tot2[...], axis=0)
    norm = row[:, 0:NB]
    corr = row[:, 16 : 16 + NB]
    square = row[:, 32 : 32 + NB]
    keep = jnp.zeros((1, NB), F32)
    for b in range(NB):
        keep = jnp.where(lane[:, :NB] == b, 1.0 - locked[b].astype(F32), keep)
    rayleigh = corr / norm
    ray_ref[...] = rayleigh
    res_ref[...] = jnp.sqrt((square - rayleigh * corr) / norm) * keep

    for part in range(2):
        drain(u_in.at[part, pl.ds(0, NY - 1)], y_send.at[part])
        drain(sent.at[part, z_others, :], z_send.at[part])
        drain(back.at[part, z_others, :], b_send.at[part])
        drain(app.at[part, :, others, :], o_send.at[part])
        drain(out.at[part, pl.ds(0, NY - 1)], o_recv.at[part])
        pltpu.make_async_copy(app.at[part, :, mine, :], out.at[part, my], o_own.at[part]).wait()
    drain(pot.at[:, others, :], y_send.at[2])
    drain(tot1.at[pl.ds(0, NZ - 1)], r_send.at[0])
    drain(tot2.at[pl.ds(0, NY - 1)], r_send.at[1])


def body(wavefunctions, potential, cutoff_sq, locked_mask):
    consts = [jnp.asarray(t) for t in tables()]
    any_space = pl.BlockSpec(memory_space=pl.ANY)
    smem = pl.BlockSpec(memory_space=pltpu.SMEM)
    vmem = pl.BlockSpec(memory_space=pltpu.VMEM)
    dma = pltpu.SemaphoreType.DMA
    applied, rayleigh, residual = pl.pallas_call(
        kernel,
        out_shape=(
            jax.ShapeDtypeStruct((2, NB, ZL, YL, N), F32),
            jax.ShapeDtypeStruct((1, NB), F32),
            jax.ShapeDtypeStruct((1, NB), F32),
        ),
        in_specs=[any_space, any_space, smem, smem] + [any_space] * 6,
        out_specs=(any_space, vmem, vmem),
        scratch_shapes=[
            pltpu.VMEM((2, NB, ZL, YL, N), F32),
            pltpu.VMEM((ZL, YL, N), F32),
            *[pltpu.VMEM(t.shape, BF16) for t in consts[:4]],
            pltpu.VMEM((4 * N, 2 * N), BF16),
            pltpu.VMEM((4 * N, 2 * N), BF16),
            pltpu.VMEM((2, ZL, N, N), F32),
            pltpu.VMEM((ZL, N, N), F32),
            pltpu.VMEM((2, NZ * BLK, N), F32),
            pltpu.VMEM((2, NZ * BLK, N), F32),
            pltpu.VMEM((2, NZ * BLK, N), F32),
            pltpu.VMEM((2, NZ * BLK, N), F32),
            pltpu.VMEM((2, ZL, N, N), F32),
            pltpu.VMEM((2 * N, 2 * N), F32),
            pltpu.VMEM((1, N), F32),
            pltpu.VMEM((1, N), F32),
            pltpu.VMEM((NZ, 1, N), F32),
            pltpu.VMEM((NY, 1, N), F32),
            dma((8,)),
            dma((3,)), dma((3,)), dma((2,)), dma((2,)), dma((2,)), dma((2,)),
            dma((2,)), dma((2,)), dma((2,)), dma((2,)), dma((2,)),
        ],
        compiler_params=pltpu.CompilerParams(collective_id=0, has_side_effects=True),
    )(wavefunctions, potential, cutoff_sq, locked_mask, *consts)
    return applied, rayleigh.reshape(NB), residual.reshape(NB)


def solution(mesh):
    placed = (P(None, None, "pz", "py", None), P("pz", "py", None), P(), P())
    return jax.shard_map(
        body,
        mesh=mesh,
        in_specs=placed,
        out_specs=(P(None, None, "pz", "py", None), P(), P()),
        check_vma=False,
    )
```

```python
import functools
import math

import jax
import jax.numpy as jnp
import numpy as np
from jax import lax
from jax.experimental import pallas as pl
from jax.experimental.pallas import tpu as pltpu
from jax.sharding import PartitionSpec as P

N = 128
NB = 8
NY = 8
NZ = 32
ZL = N // NZ
YL = N // NY
BLK = ZL * (N // NZ)
LIVE = 112
FOLD = N - LIVE
HOST = 48
SPHERE = N * N // 4
MESH = pl.DeviceIdType.MESH
F32 = jnp.float32
BF16 = jnp.bfloat16


def basis():
    n = np.arange(N)
    rows = []
    for m in range(N):
        k = (m + 1) // 2
        angle = 2.0 * np.pi * ((k * n) % N) / N
        row = np.cos(angle) if (m % 2 == 1 or m == 0) else np.sin(angle)
        scale = 1.0 / N if k in (0, N // 2) else 2.0 / N
        rows.append(np.sqrt(scale) * row)
    return np.stack(rows)


def high_low(table):
    high = table.astype(BF16)
    low = (table - high.astype(np.float64)).astype(BF16)
    return high, low


def row_order():
    hosts = [2 * k - 1 + c for k in range(HOST, HOST + FOLD // 2) for c in range(2)]
    guests = [2 * (111 - k) - 1 + c for k in range(HOST, HOST + FOLD // 2) for c in range(2)]
    plain = [m for m in range(N) if m not in hosts and m not in guests]
    for host, guest in zip(hosts, guests, strict=True):
        width = [sum(((m + 1) // 2) ** 2 + ((r + 1) // 2) ** 2 <= SPHERE for m in range(N)) for r in (host, guest)]
        assert sum(width) <= N
    return hosts + plain + guests


def tables():
    f = basis()
    fh, fl = high_low(f)
    ph, pl_ = fh[row_order()], fl[row_order()]
    right_fwd = np.block([[fh.T, fl.T], [fh.T, fl.T]])
    right_inv = np.block([[fh, fl], [fh, fl]])
    guest_fwd = np.block([[fh[::-1].T, fl[::-1].T], [fh[::-1].T, fl[::-1].T]])
    guest_inv = np.block([[fh[::-1], fl[::-1]], [fh[::-1], fl[::-1]]])
    left_fwd = np.block([[ph, ph], [pl_, pl_]])
    left_inv = np.block([[ph.T, ph.T], [pl_.T, pl_.T]])
    d = np.zeros((2, N, NZ, 2, ZL))
    for i in range(2):
        d[i, :, :, i, :] = f.reshape(N, NZ, ZL)
    d = d.reshape(2 * N, 2 * N)
    z_fwd = np.concatenate(high_low(d), axis=0)
    z_inv = np.concatenate(high_low(d.T), axis=0)
    return [right_fwd, guest_fwd, left_fwd, right_inv, guest_inv, left_inv, z_fwd, z_inv]


def split(x):
    high = x.astype(BF16)
    low = (x - high.astype(F32)).astype(BF16)
    return high, low


def dot(a, b):
    return jnp.dot(a, b, preferred_element_type=F32)


def times_right(x, table):
    high, low = split(x)
    both = dot(jnp.concatenate([high, low], axis=1), table)
    return both[:, :N] + both[:, N:]


def times_left(table, x):
    high, low = split(x)
    both = dot(table, jnp.concatenate([high, low], axis=0))
    return both[:N] + both[N:]


def times_z(table, x):
    high, low = split(x)
    both = dot(table, high)
    return both[: 2 * N] + both[2 * N :] + dot(table[: 2 * N], low)


def kernel(
    u_hbm, v_hbm, cutoff_hbm, locked_hbm, rf_hbm, gf_hbm, lf_hbm, ri_hbm, gi_hbm, li_hbm, zf_hbm, zi_hbm,
    out, ray_ref, res_ref,
    u_in, v_in, cutoff, locked, rf, gf, lf, ri, gi, li, zf, zi,
    planes, pot, sent, got, back, ret, wave, app, kin, row1, row2, tot1, tot2,
    in_sem, y_send, y_recv, z_send, z_recv, b_send, b_recv, o_send, o_recv, own, r_send, r_recv,
):
    my = lax.axis_index("py")
    mz = lax.axis_index("pz")

    y_chip = [lax.rem(my // 2 + d, 4) * 2 for d in range(4)]
    y_core = [lax.rem(my + d, 2) for d in range(2)]
    y_peers = [y_chip[d] + y_core[c] for d in (2, 1, 3, 0) for c in (0, 1) if d or c]
    z_x = [lax.rem(mz // 8 + d, 4) * 8 for d in range(4)]
    z_z = [lax.rem(mz + d, 8) for d in range(8)]
    z_peers = [(z_x[d] + z_z[e], e % 2) for e in (4, 3, 5, 2, 6, 1, 7, 0) for d in (2, 1, 3, 0) if d or e]

    def load(i, source, target):
        copy = pltpu.make_async_copy(source, target, in_sem.at[i])
        copy.start()
        return copy

    first = [load(0, u_hbm, u_in), load(1, v_hbm, v_in)]
    barrier = pltpu.get_barrier_semaphore()

    for d, _ in z_peers:
        pl.semaphore_signal(barrier, inc=1, device_id=(my, d), device_id_type=MESH)

    for j in y_peers:
        pl.semaphore_signal(barrier, inc=1, device_id=(j, mz), device_id_type=MESH)

    later = [(lf_hbm, lf), (rf_hbm, rf), (gf_hbm, gf), (cutoff_hbm, cutoff), (locked_hbm, locked), (zf_hbm, zf), (zi_hbm, zi), (ri_hbm, ri), (gi_hbm, gi), (li_hbm, li)]
    later = [load(i + 2, a, b) for i, (a, b) in enumerate(later)]
    for copy in first:
        copy.wait()
    with jax.named_scope("barrier"):
        pl.semaphore_wait(barrier, NZ - 1 + NY - 1)

    def drain(ref, sem, name="end"):
        with jax.named_scope(name):
            pltpu.make_async_copy(ref, ref, sem).wait()

    mine = pl.ds(pl.multiple_of(my * YL, YL), YL)
    for part in range(2):
        for j in y_peers:
            pltpu.make_async_remote_copy(
                u_in.at[part, j], planes.at[part, :, mine, :], y_send.at[part], y_recv.at[part],
                device_id=(j, mz), device_id_type=MESH,
            ).start()

    for j in y_peers:
        pltpu.make_async_remote_copy(
            v_in, pot.at[:, mine, :], y_send.at[2], y_recv.at[2],
            device_id=(j, mz), device_id_type=MESH,
        ).start()
    planes[:, :, mine, :] = u_in[:, my]
    pot[:, mine, :] = v_in[...]
    for copy in later:
        copy.wait()

    def first_slot(d, odd, part):
        return 7 * (d // 2) + (4 - part) * odd

    def slots(odd, part):
        return 4 - (odd + part) % 2

    lane = lax.broadcasted_iota(jnp.int32, (1, N), 1)
    up = (lane + 1) // 2
    down = (N - lane) // 2
    for part in range(2):
        start = first_slot(mz, lax.rem(mz, 2), part)
        for h in range(2):
            for i in range(2):
                slot = start + 2 * h + i
                host = slot < FOLD
                ky = jnp.where(host, HOST + slot // 2, jnp.where(slot == LIVE - 1, N // 2, (slot - FOLD + 1) // 2))
                s = ky * ky + up * up
                s = jnp.where(s > jnp.where(host, SPHERE, 4 * SPHERE), (111 - ky) * (111 - ky) + down * down, s)
                kz = (lax.broadcasted_iota(jnp.int32, (N, N), 0) + 1) // 2
                s = s + kz * kz
                kin[part, i * N : (i + 1) * N, h * N : (h + 1) * N] = jnp.where(
                    s <= cutoff[0], 0.5 * (math.pi / N) ** 2 * s.astype(F32), 0.0
                )

    others = pl.ds(0, (NY - 1) * YL)
    own_row = HOST + lax.broadcasted_iota(jnp.int32, (FOLD, N), 0) // 2
    own_kx = (lax.broadcasted_iota(jnp.int32, (FOLD, N), 1) + 1) // 2
    holds = own_row * own_row + own_kx * own_kx <= SPHERE

    def plane_transform(field, target, part):
        x = times_left(lf[...], jnp.concatenate([field[z] for z in range(ZL)], axis=1))
        x = [x[:, z * N : (z + 1) * N] for z in range(ZL)]
        guest = times_right(jnp.concatenate([a[LIVE:] for a in x], axis=0), gf[...])
        live = times_right(jnp.concatenate([a[:LIVE] for a in x], axis=0), rf[...])
        for z in range(ZL):
            a = live[z * LIVE : (z + 1) * LIVE]
            a = jnp.concatenate([jnp.where(holds, a[:FOLD], guest[z * FOLD : (z + 1) * FOLD]), a[FOLD:]], axis=0)
            target[part, pl.ds(z, LIVE, stride=ZL), :] = a

    def by_parity(act):
        for odd in range(2):
            pl.when(lax.rem(mz, 2) == odd)(functools.partial(act, odd))

    def rows(first, count, step):
        return pl.ds(pl.multiple_of(first * step, step), count * ZL)

    def z_out(part, odd):
        def copy_of(d, o):
            count = slots(o, part)
            return sent.at[part, rows(first_slot(d, o, part), count, ZL), :], got.at[part, rows(mz, count, BLK), :]

        for d, e in z_peers:
            a, b = copy_of(d, (odd + e) % 2)
            pltpu.make_async_remote_copy(
                a, b, z_send.at[part], z_recv.at[part], device_id=(my, d), device_id_type=MESH
            ).start()
        pltpu.make_async_copy(*copy_of(mz, odd), own.at[part]).start()

    def z_back(part, odd):
        count = slots(odd, part)
        target = ret.at[part, rows(first_slot(mz, odd, part), count, ZL), :]
        for d, _ in z_peers:
            pltpu.make_async_remote_copy(
                back.at[part, rows(d, count, BLK), :], target, b_send.at[part], b_recv.at[part],
                device_id=(my, d), device_id_type=MESH,
            ).start()
        pltpu.make_async_copy(back.at[part, rows(mz, count, BLK), :], target, own.at[2 + part]).start()

    def z_rows(part, odd):
        return got.at[part, pl.ds(0, (NZ - 1) * ZL * slots(odd, part)), :]

    def slot_rows(part, odd):
        return ret.at[part, pl.ds(0, ZL * (LIVE - slots(odd, part))), :]

    def z_wait(part, odd):
        drain(z_rows(part, odd), z_recv.at[part], f"z{part}")
        pltpu.make_async_copy(back.at[part, rows(0, slots(odd, part), BLK), :], got.at[part, rows(0, slots(odd, part), BLK), :], own.at[part]).wait()

    def b_wait(part, odd):
        drain(slot_rows(part, odd), b_recv.at[part], f"b{part}")
        pltpu.make_async_copy(back.at[part, rows(0, slots(odd, part), BLK), :], got.at[part, rows(0, slots(odd, part), BLK), :], own.at[2 + part]).wait()

    for part in range(2):
        drain(planes.at[part, :, others, :], y_recv.at[part], f"y{part}")
        plane_transform(planes[part], sent, part)
        by_parity(functools.partial(z_out, part))

    def folded(x):
        return jnp.sum(x.reshape(-1, 8, N), axis=0)

    drain(pot.at[:, others, :], y_recv.at[2], "pot")
    norm = corr = square = jnp.zeros((8, N), F32)
    for part in range(2):
        field = planes[part]
        local = pot[...] * field
        norm = norm + folded(field * field)
        corr = corr + folded(field * local)
        square = square + folded(local * local)
        plane_transform(local, wave, part)

    upper = lax.rem(lax.broadcasted_iota(jnp.int32, (2 * N, N), 0), 2 * ZL) < ZL
    for part in range(2):
        by_parity(functools.partial(z_wait, part))
        g = got[part].reshape(NZ, 2, 8, N)
        g = [g[:, h].reshape(2 * N, N) for h in range(2)]
        g[1] = jnp.where(upper | (lax.rem(mz + part, 2) == 0), g[1], 0.0)
        x = times_z(zf[...], jnp.concatenate(g, axis=1)) * kin[part]
        x = times_z(zi[...], x)
        x = jnp.stack([x[:, h * N : (h + 1) * N].reshape(NZ, 8, N) for h in range(2)], axis=1)
        back[part] = x.reshape(NZ * BLK, N)
        by_parity(functools.partial(z_back, part))

    for part in range(2):
        by_parity(functools.partial(b_wait, part))
        x = ret[part]
        corr = corr + folded(sent[part] * x)
        square = square + folded(x * (x + 2.0 * wave[part]))
        if part == 1:
            row = jnp.zeros((1, N), F32)
            for i, value in enumerate((norm, corr, square)):
                total = jnp.sum(jnp.sum(value, axis=0, keepdims=True), axis=1, keepdims=True)
                row = jnp.where(lane == 16 * i + my, total, row)
            row1[...] = row
            tot1[mz] = row

            for d, _ in z_peers:
                pltpu.make_async_remote_copy(
                    row1, tot1.at[mz], r_send.at[0], r_recv.at[0], device_id=(my, d), device_id_type=MESH
                ).start()

        x = [ret[part, pl.ds(z, LIVE, stride=ZL), :] for z in range(ZL)]
        guest = times_right(jnp.concatenate([jnp.where(holds, 0.0, a[:FOLD]) for a in x], axis=0), gi[...])
        live = [b for a in x for b in (jnp.where(holds, a[:FOLD], 0.0), a[FOLD:])]
        live = times_right(jnp.concatenate(live, axis=0), ri[...])
        x = [
            jnp.concatenate([live[z * LIVE : (z + 1) * LIVE], guest[z * FOLD : (z + 1) * FOLD]], axis=0)
            for z in range(ZL)
        ]
        x = times_left(li[...], jnp.concatenate(x, axis=1))
        for z in range(ZL):
            app[part, z] = x[:, z * N : (z + 1) * N] + pot[z] * planes[part, z]

        for j in y_peers:
            pltpu.make_async_remote_copy(
                app.at[part, :, pl.ds(pl.multiple_of(j * YL, YL), YL), :], out.at[part, my],
                o_send.at[part], o_recv.at[part],
                device_id=(j, mz), device_id_type=MESH,
            ).start()
        out[part, my] = app[part, :, mine, :]

    drain(tot1.at[pl.ds(0, NZ - 1)], r_recv.at[0], "r0")
    row = jnp.sum(tot1[...], axis=0)
    row2[...] = row
    tot2[my] = row

    for j in y_peers:
        pltpu.make_async_remote_copy(
            row2, tot2.at[my], r_send.at[1], r_recv.at[1], device_id=(j, mz), device_id_type=MESH
        ).start()

    for part in range(2):
        drain(u_in.at[part, pl.ds(0, NY - 1)], y_send.at[part])
        by_parity(lambda odd, part=part: drain(slot_rows(part, odd), z_send.at[part]))
        by_parity(lambda odd, part=part: drain(z_rows(part, odd), b_send.at[part]))
        drain(app.at[part, :, others, :], o_send.at[part])
        drain(out.at[part, pl.ds(0, NY - 1)], o_recv.at[part], f"o{part}")
    drain(pot.at[:, others, :], y_send.at[2])
    drain(tot1.at[pl.ds(0, NZ - 1)], r_send.at[0])

    keep = jnp.zeros((1, NB), F32)
    for b in range(NB):
        keep = jnp.where(lane[:, :NB] == b, 1.0 - locked[b].astype(F32), keep)
    drain(tot2.at[pl.ds(0, NY - 1)], r_recv.at[1], "r1")
    row = jnp.sum(tot2[...], axis=0)
    norm = row[:, 0:NB]
    corr = row[:, 16 : 16 + NB]
    square = row[:, 32 : 32 + NB]
    rayleigh = corr / norm
    ray_ref[...] = rayleigh.reshape(NB)
    res_ref[...] = (jnp.sqrt((square - rayleigh * corr) / norm) * keep).reshape(NB)
    drain(tot2.at[pl.ds(0, NY - 1)], r_send.at[1])


def write_out(applied, rayleigh, residual, *rest):
    sources, sem = (applied, rayleigh, residual), rest[3]
    copies = [pltpu.make_async_copy(a, b, sem.at[i]) for i, (a, b) in enumerate(zip(sources, rest[:3], strict=True))]
    for copy in copies:
        copy.start()
    for copy in copies:
        copy.wait()


def body(wavefunctions, potential, cutoff_sq, locked_mask):
    consts = [jnp.asarray(t) for t in tables()]
    hbm = pl.BlockSpec(memory_space=pltpu.HBM)
    vmem = pl.BlockSpec(memory_space=pltpu.VMEM)
    dma = pltpu.SemaphoreType.DMA
    applied, rayleigh, residual = pl.pallas_call(
        kernel,
        out_shape=(
            pltpu.VMEM((2, NB, ZL, YL, N), F32),
            pltpu.VMEM((NB,), F32),
            pltpu.VMEM((NB,), F32),
        ),
        in_specs=[hbm] * 12,
        out_specs=(vmem, vmem, vmem),
        scratch_shapes=[
            pltpu.VMEM((2, NB, ZL, YL, N), F32),
            pltpu.VMEM((ZL, YL, N), F32),
            pltpu.SMEM((1,), jnp.int32),
            pltpu.SMEM((NB,), jnp.int32),
            *[pltpu.VMEM(t.shape, BF16) for t in consts],
            pltpu.VMEM((2, ZL, N, N), F32),
            pltpu.VMEM((ZL, N, N), F32),
            pltpu.VMEM((2, LIVE * ZL, N), F32),
            pltpu.VMEM((2, NZ * BLK, N), F32),
            pltpu.VMEM((2, NZ * BLK, N), F32),
            pltpu.VMEM((2, LIVE * ZL, N), F32),
            pltpu.VMEM((2, LIVE * ZL, N), F32),
            pltpu.VMEM((2, ZL, N, N), F32),
            pltpu.VMEM((2, 2 * N, 2 * N), F32),
            pltpu.VMEM((1, N), F32),
            pltpu.VMEM((1, N), F32),
            pltpu.VMEM((NZ, 1, N), F32),
            pltpu.VMEM((NY, 1, N), F32),
            dma((12,)),
            dma((3,)), dma((3,)), dma((2,)), dma((2,)), dma((2,)), dma((2,)),
            dma((2,)), dma((2,)), dma((4,)), dma((2,)), dma((2,)),
        ],
        compiler_params=pltpu.CompilerParams(collective_id=0, has_side_effects=True),
    )(wavefunctions, potential, cutoff_sq, locked_mask, *consts)
    return pl.pallas_call(
        write_out,
        out_shape=(
            jax.ShapeDtypeStruct((2, NB, ZL, YL, N), F32),
            jax.ShapeDtypeStruct((NB,), F32),
            jax.ShapeDtypeStruct((NB,), F32),
        ),
        in_specs=[vmem] * 3,
        out_specs=(hbm,) * 3,
        scratch_shapes=[dma((3,))],
    )(*[pltpu.with_memory_space_constraint(a, pltpu.VMEM) for a in (applied, rayleigh, residual)])


def solution(mesh):
    placed = (P(None, None, "pz", "py", None), P("pz", "py", None), P(), P())
    return jax.shard_map(
        body,
        mesh=mesh,
        in_specs=placed,
        out_specs=(P(None, None, "pz", "py", None), P(), P()),
        check_vma=False,
    )
```

```python
import functools
import math

import jax
import jax.numpy as jnp
import numpy as np
from jax import lax
from jax.experimental import pallas as pl
from jax.experimental.pallas import tpu as pltpu
from jax.sharding import PartitionSpec as P

N = 128
NB = 8
NY = 8
NZ = 32
ZL = N // NZ
YL = N // NY
SL = N // NZ
CHUNKS = ((0, 0, 1), (0, 1, 1), (0, 2, 2), (1, 0, 4))
LIVE = 112
FOLD = N - LIVE
HOST = 48
SPHERE = N * N // 4
MESH = pl.DeviceIdType.MESH
F32 = jnp.float32
BF16 = jnp.bfloat16


def basis():
    n = np.arange(N)
    rows = []
    for m in range(N):
        k = (m + 1) // 2
        angle = 2.0 * np.pi * ((k * n) % N) / N
        row = np.cos(angle) if (m % 2 == 1 or m == 0) else np.sin(angle)
        scale = 1.0 / N if k in (0, N // 2) else 2.0 / N
        rows.append(np.sqrt(scale) * row)
    return np.stack(rows)


def high_low(table):
    high = table.astype(BF16)
    low = (table - high.astype(np.float64)).astype(BF16)
    return high, low


def row_order():
    hosts = [2 * k - 1 + c for k in range(HOST, HOST + FOLD // 2) for c in range(2)]
    guests = [2 * (111 - k) - 1 + c for k in range(HOST, HOST + FOLD // 2) for c in range(2)]
    plain = [m for m in range(N) if m not in hosts and m not in guests]
    for host, guest in zip(hosts, guests, strict=True):
        width = [sum(((m + 1) // 2) ** 2 + ((r + 1) // 2) ** 2 <= SPHERE for m in range(N)) for r in (host, guest)]
        assert sum(width) <= N
    return hosts + plain + guests


def tables():
    f = basis()
    fh, fl = high_low(f)
    ph, pl_ = fh[row_order()], fl[row_order()]
    right_fwd = np.block([[fh.T, fl.T], [fh.T, fl.T]])
    right_inv = np.block([[fh, fl], [fh, fl]])
    guest_fwd = np.block([[fh[::-1].T, fl[::-1].T], [fh[::-1].T, fl[::-1].T]])
    guest_inv = np.block([[fh[::-1], fl[::-1]], [fh[::-1], fl[::-1]]])
    left_fwd = np.block([[ph, ph], [pl_, pl_]])
    left_inv = np.block([[ph.T, ph.T], [pl_.T, pl_.T]])
    zh, zl = (t.reshape(N, NZ, ZL).swapaxes(1, 2).reshape(N, N) for t in (fh, fl))
    z_fwd = np.block([[zh, zh], [zl, zl]])
    z_inv = np.block([[zh.T, zh.T], [zl.T, zl.T]])
    return [right_fwd, guest_fwd, left_fwd, right_inv, guest_inv, left_inv, z_fwd, z_inv]


def split(x):
    high = x.astype(BF16)
    low = (x - high.astype(F32)).astype(BF16)
    return high, low


def dot(a, b):
    return jnp.dot(a, b, preferred_element_type=F32)


def times_right(x, table):
    high, low = split(x)
    both = dot(jnp.concatenate([high, low], axis=1), table)
    return both[:, :N] + both[:, N:]


def times_left(table, x):
    high, low = split(x)
    both = dot(table, jnp.concatenate([high, low], axis=0))
    return both[:N] + both[N:]


def kernel(
    u_hbm, v_hbm, cutoff_hbm, locked_hbm, rf_hbm, gf_hbm, lf_hbm, ri_hbm, gi_hbm, li_hbm, zf_hbm, zi_hbm,
    out, ray_ref, res_ref,
    u_in, v_in, cutoff, locked, rf, gf, lf, ri, gi, li, zf, zi,
    planes, pot, sent, got, back, ret, wave, app, kin, row1, row2, tot1, tot2,
    in_sem, y_send, y_recv, z_send, z_recv, b_send, b_recv, o_send, o_recv, own, r_send, r_recv,
):
    my = lax.axis_index("py")
    mz = lax.axis_index("pz")

    y_chip = [lax.rem(my // 2 + d, 4) * 2 for d in range(4)]
    y_core = [lax.rem(my + d, 2) for d in range(2)]
    y_peers = [y_chip[d] + y_core[c] for d in (2, 1, 3, 0) for c in (0, 1) if d or c]
    z_x = [lax.rem(mz // 8 + d, 4) * 8 for d in range(4)]
    z_z = [lax.rem(mz + d, 8) for d in range(8)]
    z_peers = [(z_x[d] + z_z[e], e % 2) for e in (4, 3, 5, 2, 6, 1, 7, 0) for d in (2, 1, 3, 0) if d or e]

    def load(i, source, target):
        copy = pltpu.make_async_copy(source, target, in_sem.at[i])
        copy.start()
        return copy

    first = [load(0, u_hbm, u_in), load(1, v_hbm, v_in)]
    barrier = pltpu.get_barrier_semaphore()

    for d, _ in z_peers:
        pl.semaphore_signal(barrier, inc=1, device_id=(my, d), device_id_type=MESH)

    for j in y_peers:
        pl.semaphore_signal(barrier, inc=1, device_id=(j, mz), device_id_type=MESH)

    later = [(lf_hbm, lf), (rf_hbm, rf), (gf_hbm, gf), (cutoff_hbm, cutoff), (locked_hbm, locked), (zf_hbm, zf), (zi_hbm, zi), (ri_hbm, ri), (gi_hbm, gi), (li_hbm, li)]
    later = [load(i + 2, a, b) for i, (a, b) in enumerate(later)]
    for copy in first:
        copy.wait()
    with jax.named_scope("barrier"):
        pl.semaphore_wait(barrier, NZ - 1 + NY - 1)

    def drain(ref, sem, name="end"):
        with jax.named_scope(name):
            pltpu.make_async_copy(ref, ref, sem).wait()

    mine = pl.ds(pl.multiple_of(my * YL, YL), YL)
    for c, (part, z, nz) in enumerate(CHUNKS):
        for j in y_peers:
            pltpu.make_async_remote_copy(
                u_in.at[part, j, pl.ds(z, nz)], planes.at[part, pl.ds(z, nz), mine, :], y_send.at[c], y_recv.at[c],
                device_id=(j, mz), device_id_type=MESH,
            ).start()

    for j in y_peers:
        pltpu.make_async_remote_copy(
            v_in, pot.at[:, mine, :], y_send.at[len(CHUNKS)], y_recv.at[len(CHUNKS)],
            device_id=(j, mz), device_id_type=MESH,
        ).start()
    planes[:, :, mine, :] = u_in[:, my]
    pot[:, mine, :] = v_in[...]
    for copy in later:
        copy.wait()

    def first_slot(d, odd, part):
        return 7 * (d // 2) + (4 - part) * odd

    def slots(odd, part):
        return 4 - (odd + part) % 2

    lane = lax.broadcasted_iota(jnp.int32, (1, N), 1)
    up = (lane + 1) // 2
    down = (N - lane) // 2
    for part in range(2):
        start = first_slot(mz, lax.rem(mz, 2), part)
        for i in range(SL):
            slot = start + i
            host = slot < FOLD
            ky = jnp.where(host, HOST + slot // 2, jnp.where(slot == LIVE - 1, N // 2, (slot - FOLD + 1) // 2))
            s = ky * ky + up * up
            s = jnp.where(s > jnp.where(host, SPHERE, 4 * SPHERE), (111 - ky) * (111 - ky) + down * down, s)
            kz = (lax.broadcasted_iota(jnp.int32, (N, N), 0) + 1) // 2
            s = s + kz * kz
            kin[part, :, i * N : (i + 1) * N] = jnp.where(
                s <= cutoff[0], 0.5 * (math.pi / N) ** 2 * s.astype(F32), 0.0
            )

    others = pl.ds(0, (NY - 1) * YL)
    own_row = HOST + lax.broadcasted_iota(jnp.int32, (FOLD, N), 0) // 2
    own_kx = (lax.broadcasted_iota(jnp.int32, (FOLD, N), 1) + 1) // 2
    holds = own_row * own_row + own_kx * own_kx <= SPHERE

    def plane_transform(field, target, part, first, count):
        x = times_left(lf[...], jnp.concatenate([field[z] for z in range(count)], axis=1))
        x = [x[:, z * N : (z + 1) * N] for z in range(count)]
        guest = times_right(jnp.concatenate([a[LIVE:] for a in x], axis=0), gf[...])
        live = times_right(jnp.concatenate([a[:LIVE] for a in x], axis=0), rf[...])
        for z in range(count):
            a = live[z * LIVE : (z + 1) * LIVE]
            target[part, first + z, :FOLD, :] = jnp.where(holds, a[:FOLD], guest[z * FOLD : (z + 1) * FOLD])
            target[part, first + z, FOLD:, :] = a[FOLD:]

    def by_parity(act):
        for odd in range(2):
            pl.when(lax.rem(mz, 2) == odd)(functools.partial(act, odd))

    got_view = got.reshape(2, NZ, ZL, SL, N)
    back_view = back.reshape(2, NZ, ZL, SL, N)

    def z_out(part, first, count, c, odd):
        def copy_of(d, o):
            n = slots(o, part)
            return (
                sent.at[part, pl.ds(first, count), pl.ds(first_slot(d, o, part), n), :],
                got_view.at[part, mz, pl.ds(first, count), pl.ds(0, n), :],
            )

        for d, e in z_peers:
            a, b = copy_of(d, (odd + e) % 2)
            pltpu.make_async_remote_copy(
                a, b, z_send.at[part], z_recv.at[part], device_id=(my, d), device_id_type=MESH
            ).start()
        pltpu.make_async_copy(*copy_of(mz, odd), own.at[c]).start()

    def z_back(part, odd):
        n = slots(odd, part)
        target = ret.at[part, :, pl.ds(first_slot(mz, odd, part), n), :]
        for d, _ in z_peers:
            pltpu.make_async_remote_copy(
                back_view.at[part, d, :, pl.ds(0, n), :], target, b_send.at[part], b_recv.at[part],
                device_id=(my, d), device_id_type=MESH,
            ).start()
        pltpu.make_async_copy(back_view.at[part, mz, :, pl.ds(0, n), :], target, own.at[len(CHUNKS) + part]).start()

    def z_rows(part, odd):
        return got_view.at[part, pl.ds(0, NZ - 1), :, pl.ds(0, slots(odd, part)), :]

    def slot_rows(part, odd):
        return ret.at[part, :, pl.ds(0, LIVE - slots(odd, part)), :]

    def own_wait(part, count, c, odd):
        a = ret.at[part, pl.ds(0, count), pl.ds(0, slots(odd, part)), :]
        pltpu.make_async_copy(a, a, own.at[c]).wait()

    def z_wait(part, odd):
        drain(z_rows(part, odd), z_recv.at[part], f"z{part}")
        for c, (p, _, count) in enumerate(CHUNKS):
            if p == part:
                own_wait(part, count, c, odd)

    def b_wait(part, odd):
        drain(slot_rows(part, odd), b_recv.at[part], f"b{part}")
        own_wait(part, ZL, len(CHUNKS) + part, odd)

    for c, (part, z, nz) in enumerate(CHUNKS):
        drain(planes.at[part, pl.ds(z, nz), others, :], y_recv.at[c], f"y{c}")
        plane_transform(planes[part, z : z + nz], sent, part, z, nz)
        by_parity(functools.partial(z_out, part, z, nz, c))

    def folded(x):
        return jnp.sum(x.reshape(-1, 8, N), axis=0)

    drain(pot.at[:, others, :], y_recv.at[len(CHUNKS)], "pot")
    norm = corr = square = jnp.zeros((8, N), F32)
    for part in range(2):
        field = planes[part]
        local = pot[...] * field
        norm = norm + folded(field * field)
        corr = corr + folded(field * local)
        square = square + folded(local * local)
        plane_transform(local, wave, part, 0, ZL)

    for part in range(2):
        by_parity(functools.partial(z_wait, part))
        x = [
            jnp.concatenate([got[part, pl.ds(SL * z + i, NZ, stride=SL * ZL), :] for z in range(ZL)], axis=0)
            for i in range(SL)
        ]
        x = times_left(zf[...], jnp.concatenate(x, axis=1)) * kin[part]
        x = times_left(zi[...], x)
        for z in range(ZL):
            for i in range(SL):
                back[part, pl.ds(SL * z + i, NZ, stride=SL * ZL), :] = x[z * NZ : (z + 1) * NZ, i * N : (i + 1) * N]
        by_parity(functools.partial(z_back, part))

    for part in range(2):
        by_parity(functools.partial(b_wait, part))
        x = ret[part]
        corr = corr + folded(sent[part] * x)
        square = square + folded(x * (x + 2.0 * wave[part]))
        if part == 1:
            row = jnp.zeros((1, N), F32)
            for i, value in enumerate((norm, corr, square)):
                total = jnp.sum(jnp.sum(value, axis=0, keepdims=True), axis=1, keepdims=True)
                row = jnp.where(lane == 16 * i + my, total, row)
            row1[...] = row
            tot1[mz] = row

            for d, _ in z_peers:
                pltpu.make_async_remote_copy(
                    row1, tot1.at[mz], r_send.at[0], r_recv.at[0], device_id=(my, d), device_id_type=MESH
                ).start()

        x = [ret[part, z] for z in range(ZL)]
        guest = times_right(jnp.concatenate([jnp.where(holds, 0.0, a[:FOLD]) for a in x], axis=0), gi[...])
        live = [b for a in x for b in (jnp.where(holds, a[:FOLD], 0.0), a[FOLD:])]
        live = times_right(jnp.concatenate(live, axis=0), ri[...])
        x = [
            jnp.concatenate([live[z * LIVE : (z + 1) * LIVE], guest[z * FOLD : (z + 1) * FOLD]], axis=0)
            for z in range(ZL)
        ]
        x = times_left(li[...], jnp.concatenate(x, axis=1))
        for z in range(ZL):
            app[part, z] = x[:, z * N : (z + 1) * N] + pot[z] * planes[part, z]

        for j in y_peers:
            pltpu.make_async_remote_copy(
                app.at[part, :, pl.ds(pl.multiple_of(j * YL, YL), YL), :], out.at[part, my],
                o_send.at[part], o_recv.at[part],
                device_id=(j, mz), device_id_type=MESH,
            ).start()
        out[part, my] = app[part, :, mine, :]

    drain(tot1.at[pl.ds(0, NZ - 1)], r_recv.at[0], "r0")
    row = jnp.sum(tot1[...], axis=0)
    row2[...] = row
    tot2[my] = row

    for j in y_peers:
        pltpu.make_async_remote_copy(
            row2, tot2.at[my], r_send.at[1], r_recv.at[1], device_id=(j, mz), device_id_type=MESH
        ).start()

    for part in range(2):
        by_parity(lambda odd, part=part: drain(slot_rows(part, odd), z_send.at[part]))
        by_parity(lambda odd, part=part: drain(z_rows(part, odd), b_send.at[part]))
        drain(app.at[part, :, others, :], o_send.at[part])
        drain(out.at[part, pl.ds(0, NY - 1)], o_recv.at[part], f"o{part}")
    drain(pot.at[:, others, :], y_send.at[len(CHUNKS)])
    for c, (part, z, nz) in enumerate(CHUNKS):
        drain(planes.at[part, pl.ds(z, nz), others, :], y_send.at[c])
    drain(tot1.at[pl.ds(0, NZ - 1)], r_send.at[0])

    keep = jnp.zeros((1, NB), F32)
    for b in range(NB):
        keep = jnp.where(lane[:, :NB] == b, 1.0 - locked[b].astype(F32), keep)
    drain(tot2.at[pl.ds(0, NY - 1)], r_recv.at[1], "r1")
    row = jnp.sum(tot2[...], axis=0)
    norm = row[:, 0:NB]
    corr = row[:, 16 : 16 + NB]
    square = row[:, 32 : 32 + NB]
    rayleigh = corr / norm
    ray_ref[...] = rayleigh.reshape(NB)
    res_ref[...] = (jnp.sqrt((square - rayleigh * corr) / norm) * keep).reshape(NB)
    drain(tot2.at[pl.ds(0, NY - 1)], r_send.at[1])


def write_out(applied, rayleigh, residual, *rest):
    sources, sem = (applied, rayleigh, residual), rest[3]
    copies = [pltpu.make_async_copy(a, b, sem.at[i]) for i, (a, b) in enumerate(zip(sources, rest[:3], strict=True))]
    for copy in copies:
        copy.start()
    for copy in copies:
        copy.wait()


def body(wavefunctions, potential, cutoff_sq, locked_mask):
    consts = [jnp.asarray(t) for t in tables()]
    hbm = pl.BlockSpec(memory_space=pltpu.HBM)
    vmem = pl.BlockSpec(memory_space=pltpu.VMEM)
    dma = pltpu.SemaphoreType.DMA
    applied, rayleigh, residual = pl.pallas_call(
        kernel,
        out_shape=(
            pltpu.VMEM((2, NB, ZL, YL, N), F32),
            pltpu.VMEM((NB,), F32),
            pltpu.VMEM((NB,), F32),
        ),
        in_specs=[hbm] * 12,
        out_specs=(vmem, vmem, vmem),
        scratch_shapes=[
            pltpu.VMEM((2, NB, ZL, YL, N), F32),
            pltpu.VMEM((ZL, YL, N), F32),
            pltpu.SMEM((1,), jnp.int32),
            pltpu.SMEM((NB,), jnp.int32),
            *[pltpu.VMEM(t.shape, BF16) for t in consts],
            pltpu.VMEM((2, ZL, N, N), F32),
            pltpu.VMEM((ZL, N, N), F32),
            pltpu.VMEM((2, ZL, LIVE, N), F32),
            pltpu.VMEM((2, NZ * ZL * SL, N), F32),
            pltpu.VMEM((2, NZ * ZL * SL, N), F32),
            pltpu.VMEM((2, ZL, LIVE, N), F32),
            pltpu.VMEM((2, ZL, LIVE, N), F32),
            pltpu.VMEM((2, ZL, N, N), F32),
            pltpu.VMEM((2, N, SL * N), F32),
            pltpu.VMEM((1, N), F32),
            pltpu.VMEM((1, N), F32),
            pltpu.VMEM((NZ, 1, N), F32),
            pltpu.VMEM((NY, 1, N), F32),
            dma((12,)),
            dma((len(CHUNKS) + 1,)), dma((len(CHUNKS) + 1,)), dma((2,)), dma((2,)), dma((2,)), dma((2,)),
            dma((2,)), dma((2,)), dma((len(CHUNKS) + 2,)), dma((2,)), dma((2,)),
        ],
        compiler_params=pltpu.CompilerParams(collective_id=0, has_side_effects=True),
    )(wavefunctions, potential, cutoff_sq, locked_mask, *consts)
    return pl.pallas_call(
        write_out,
        out_shape=(
            jax.ShapeDtypeStruct((2, NB, ZL, YL, N), F32),
            jax.ShapeDtypeStruct((NB,), F32),
            jax.ShapeDtypeStruct((NB,), F32),
        ),
        in_specs=[vmem] * 3,
        out_specs=(hbm,) * 3,
        scratch_shapes=[dma((3,))],
    )(*[pltpu.with_memory_space_constraint(a, pltpu.VMEM) for a in (applied, rayleigh, residual)])


def solution(mesh):
    placed = (P(None, None, "pz", "py", None), P("pz", "py", None), P(), P())
    return jax.shard_map(
        body,
        mesh=mesh,
        in_specs=placed,
        out_specs=(P(None, None, "pz", "py", None), P(), P()),
        check_vma=False,
    )
```

```python
import functools
import math

import jax
import jax.numpy as jnp
import numpy as np
from jax import lax
from jax.experimental import pallas as pl
from jax.experimental.pallas import tpu as pltpu
from jax.sharding import PartitionSpec as P

N = 128
NB = 8
NY = 8
NZ = 32
ZL = N // NZ
YL = N // NY
ENTRY = ((0, 2), (0, 6), (2, 0), (1, 1), (1, 7), (3, 1), (3, 7), (1, 0), (3, 0), (0, 1), (0, 7))
ROUNDS = (((0, 2), (0, 6), (2, 0)), ((0, 2), (0, 6)))
SENT_IN = ((0, 1, 2, 3), (), ())
SL = N // NZ
CHUNKS = ((0, 0, 1), (0, 1, 1), (0, 2, 2), (1, 0, 4))
LIVE = 112
FOLD = N - LIVE
HOST = 48
SPHERE = N * N // 4
MESH = pl.DeviceIdType.MESH
F32 = jnp.float32
BF16 = jnp.bfloat16


def basis():
    n = np.arange(N)
    rows = []
    for m in range(N):
        k = (m + 1) // 2
        angle = 2.0 * np.pi * ((k * n) % N) / N
        row = np.cos(angle) if (m % 2 == 1 or m == 0) else np.sin(angle)
        scale = 1.0 / N if k in (0, N // 2) else 2.0 / N
        rows.append(np.sqrt(scale) * row)
    return np.stack(rows)


def high_low(table):
    high = table.astype(BF16)
    low = (table - high.astype(np.float64)).astype(BF16)
    return high, low


def row_order():
    hosts = [2 * k - 1 + c for k in range(HOST, HOST + FOLD // 2) for c in range(2)]
    guests = [2 * (111 - k) - 1 + c for k in range(HOST, HOST + FOLD // 2) for c in range(2)]
    plain = [m for m in range(N) if m not in hosts and m not in guests]
    for host, guest in zip(hosts, guests, strict=True):
        width = [sum(((m + 1) // 2) ** 2 + ((r + 1) // 2) ** 2 <= SPHERE for m in range(N)) for r in (host, guest)]
        assert sum(width) <= N
    return hosts + plain + guests


def tables():
    f = basis()
    fh, fl = high_low(f)
    ph, pl_ = fh[row_order()], fl[row_order()]
    right_fwd = np.block([[fh.T, fl.T], [fh.T, fl.T]])
    right_inv = np.block([[fh, fl], [fh, fl]])
    guest_fwd = np.block([[fh[::-1].T, fl[::-1].T], [fh[::-1].T, fl[::-1].T]])
    guest_inv = np.block([[fh[::-1], fl[::-1]], [fh[::-1], fl[::-1]]])
    left_fwd = np.block([[ph, ph], [pl_, pl_]])
    left_inv = np.block([[ph.T, ph.T], [pl_.T, pl_.T]])
    zh, zl = (t.reshape(N, NZ, ZL).swapaxes(1, 2).reshape(N, N) for t in (fh, fl))
    z_fwd = np.block([[zh, zh], [zl, zl]])
    z_inv = np.block([[zh.T, zh.T], [zl.T, zl.T]])
    return [right_fwd, guest_fwd, left_fwd, right_inv, guest_inv, left_inv, z_fwd, z_inv]


def split(x):
    high = x.astype(BF16)
    low = (x - high.astype(F32)).astype(BF16)
    return high, low


def dot(a, b):
    return jnp.dot(a, b, preferred_element_type=F32)


def times_right(x, table):
    high, low = split(x)
    both = dot(jnp.concatenate([high, low], axis=1), table)
    return both[:, :N] + both[:, N:]


def times_left(table, x):
    high, low = split(x)
    both = dot(table, jnp.concatenate([high, low], axis=0))
    return both[:N] + both[N:]


def kernel(
    u_hbm, v_hbm, cutoff_hbm, locked_hbm, rf_hbm, gf_hbm, lf_hbm, ri_hbm, gi_hbm, li_hbm, zf_hbm, zi_hbm,
    out, ray_ref, res_ref,
    u_in, v_in, cutoff, locked, rf, gf, lf, ri, gi, li, zf, zi,
    planes, pot, sent, got, back, ret, wave, app, kin, row1, row2, tot1, tot2,
    in_sem, y_send, y_recv, z_send, z_recv, b_send, b_recv, o_send, o_recv, own, r_send, r_recv, rounds,
):
    my = lax.axis_index("py")
    mz = lax.axis_index("pz")

    y_chip = [lax.rem(my // 2 + d, 4) * 2 for d in range(4)]
    y_core = [lax.rem(my + d, 2) for d in range(2)]
    y_peers = [y_chip[d] + y_core[c] for d in (2, 1, 3, 0) for c in (0, 1) if d or c]
    z_x = [lax.rem(mz // 8 + d, 4) * 8 for d in range(4)]
    z_z = [lax.rem(mz + d, 8) for d in range(8)]
    z_peers = [(z_x[d] + z_z[e], e % 2) for d in (2, 1, 3, 0) for e in (4, 3, 5, 2, 6, 1, 7, 0) if d or e]

    def load(i, source, target):
        copy = pltpu.make_async_copy(source, target, in_sem.at[i])
        copy.start()
        return copy

    first = [load(0, u_hbm, u_in), load(1, v_hbm, v_in)]
    barrier = pltpu.get_barrier_semaphore()

    def greet(sem, offsets):
        for d, e in offsets:
            pl.semaphore_signal(sem, inc=1, device_id=(my, z_x[d] + z_z[e]), device_id_type=MESH)

    greet(barrier, ENTRY)
    for j in y_peers:
        pl.semaphore_signal(barrier, inc=1, device_id=(j, mz), device_id_type=MESH)

    later = [(lf_hbm, lf), (rf_hbm, rf), (gf_hbm, gf), (cutoff_hbm, cutoff), (locked_hbm, locked), (zf_hbm, zf), (zi_hbm, zi), (ri_hbm, ri), (gi_hbm, gi), (li_hbm, li)]
    later = [load(i + 2, a, b) for i, (a, b) in enumerate(later)]
    for copy in first:
        copy.wait()
    with jax.named_scope("barrier"):
        pl.semaphore_wait(barrier, len(ENTRY) + NY - 1)

    def drain(ref, sem, name="end"):
        with jax.named_scope(name):
            pltpu.make_async_copy(ref, ref, sem).wait()

    mine = pl.ds(pl.multiple_of(my * YL, YL), YL)
    def y_out(c):
        part, z, nz = CHUNKS[c]
        for j in y_peers:
            pltpu.make_async_remote_copy(
                u_in.at[part, j, pl.ds(z, nz)], planes.at[part, pl.ds(z, nz), mine, :], y_send.at[c], y_recv.at[c],
                device_id=(j, mz), device_id_type=MESH,
            ).start()

    for r, offsets in enumerate(ROUNDS):
        if r:
            with jax.named_scope(f"round{r}"):
                pl.semaphore_wait(rounds.at[r - 1], len(ROUNDS[r - 1]))
        greet(rounds.at[r], offsets)
        for c in SENT_IN[r]:
            y_out(c)
    with jax.named_scope("roundlast"):
        pl.semaphore_wait(rounds.at[len(ROUNDS) - 1], len(ROUNDS[-1]))
    for c in SENT_IN[len(ROUNDS)]:
        y_out(c)
    for j in y_peers:
        pltpu.make_async_remote_copy(
            v_in, pot.at[:, mine, :], y_send.at[len(CHUNKS)], y_recv.at[len(CHUNKS)],
            device_id=(j, mz), device_id_type=MESH,
        ).start()
    planes[:, :, mine, :] = u_in[:, my]
    pot[:, mine, :] = v_in[...]
    for copy in later:
        copy.wait()

    def first_slot(d, odd, part):
        return 7 * (d // 2) + (4 - part) * odd

    def slots(odd, part):
        return 4 - (odd + part) % 2

    lane = lax.broadcasted_iota(jnp.int32, (1, N), 1)
    up = (lane + 1) // 2
    down = (N - lane) // 2
    others = pl.ds(0, (NY - 1) * YL)
    own_row = HOST + lax.broadcasted_iota(jnp.int32, (FOLD, N), 0) // 2
    own_kx = (lax.broadcasted_iota(jnp.int32, (FOLD, N), 1) + 1) // 2
    holds = own_row * own_row + own_kx * own_kx <= SPHERE

    def plane_transform(field, target, part, first, count):
        x = times_left(lf[...], jnp.concatenate([field[z] for z in range(count)], axis=1))
        x = [x[:, z * N : (z + 1) * N] for z in range(count)]
        guest = times_right(jnp.concatenate([a[LIVE:] for a in x], axis=0), gf[...])
        live = times_right(jnp.concatenate([a[:LIVE] for a in x], axis=0), rf[...])
        for z in range(count):
            a = live[z * LIVE : (z + 1) * LIVE]
            target[part, first + z, :FOLD, :] = jnp.where(holds, a[:FOLD], guest[z * FOLD : (z + 1) * FOLD])
            target[part, first + z, FOLD:, :] = a[FOLD:]

    def by_parity(act):
        for odd in range(2):
            pl.when(lax.rem(mz, 2) == odd)(functools.partial(act, odd))

    got_view = got.reshape(2, NZ, ZL, SL, N)
    back_view = back.reshape(2, NZ, ZL, SL, N)

    def z_out(part, first, count, c, odd):
        def copy_of(d, o):
            n = slots(o, part)
            return (
                sent.at[part, pl.ds(first, count), pl.ds(first_slot(d, o, part), n), :],
                got_view.at[part, mz, pl.ds(first, count), pl.ds(0, n), :],
            )

        for d, e in z_peers:
            a, b = copy_of(d, (odd + e) % 2)
            pltpu.make_async_remote_copy(
                a, b, z_send.at[part], z_recv.at[part], device_id=(my, d), device_id_type=MESH
            ).start()
        pltpu.make_async_copy(*copy_of(mz, odd), own.at[c]).start()

    def z_back(part, odd):
        n = slots(odd, part)
        target = ret.at[part, :, pl.ds(first_slot(mz, odd, part), n), :]
        for d, _ in z_peers:
            pltpu.make_async_remote_copy(
                back_view.at[part, d, :, pl.ds(0, n), :], target, b_send.at[part], b_recv.at[part],
                device_id=(my, d), device_id_type=MESH,
            ).start()
        pltpu.make_async_copy(back_view.at[part, mz, :, pl.ds(0, n), :], target, own.at[len(CHUNKS) + part]).start()

    def z_rows(part, odd):
        return got_view.at[part, pl.ds(0, NZ - 1), :, pl.ds(0, slots(odd, part)), :]

    def slot_rows(part, odd):
        return ret.at[part, :, pl.ds(0, LIVE - slots(odd, part)), :]

    def own_wait(part, count, c, odd):
        a = ret.at[part, pl.ds(0, count), pl.ds(0, slots(odd, part)), :]
        pltpu.make_async_copy(a, a, own.at[c]).wait()

    def z_wait(part, odd):
        drain(z_rows(part, odd), z_recv.at[part], f"z{part}")
        for c, (p, _, count) in enumerate(CHUNKS):
            if p == part:
                own_wait(part, count, c, odd)

    def b_wait(part, odd):
        drain(slot_rows(part, odd), b_recv.at[part], f"b{part}")
        own_wait(part, ZL, len(CHUNKS) + part, odd)

    for c, (part, z, nz) in enumerate(CHUNKS):
        drain(planes.at[part, pl.ds(z, nz), others, :], y_recv.at[c], f"y{c}")
        plane_transform(planes[part, z : z + nz], sent, part, z, nz)
        by_parity(functools.partial(z_out, part, z, nz, c))

    for part in range(2):
        start = first_slot(mz, lax.rem(mz, 2), part)
        for i in range(SL):
            slot = start + i
            host = slot < FOLD
            ky = jnp.where(host, HOST + slot // 2, jnp.where(slot == LIVE - 1, N // 2, (slot - FOLD + 1) // 2))
            s = ky * ky + up * up
            s = jnp.where(s > jnp.where(host, SPHERE, 4 * SPHERE), (111 - ky) * (111 - ky) + down * down, s)
            kz = (lax.broadcasted_iota(jnp.int32, (N, N), 0) + 1) // 2
            s = s + kz * kz
            kin[part, :, i * N : (i + 1) * N] = jnp.where(
                s <= cutoff[0], 0.5 * (math.pi / N) ** 2 * s.astype(F32), 0.0
            )

    def folded(x):
        return jnp.sum(x.reshape(-1, 8, N), axis=0)

    drain(pot.at[:, others, :], y_recv.at[len(CHUNKS)], "pot")
    norm = corr = square = jnp.zeros((8, N), F32)
    for part in range(2):
        field = planes[part]
        local = pot[...] * field
        norm = norm + folded(field * field)
        corr = corr + folded(field * local)
        square = square + folded(local * local)
        plane_transform(local, wave, part, 0, ZL)

    for part in range(2):
        by_parity(functools.partial(z_wait, part))
        x = [
            jnp.concatenate([got[part, pl.ds(SL * z + i, NZ, stride=SL * ZL), :] for z in range(ZL)], axis=0)
            for i in range(SL)
        ]
        x = times_left(zf[...], jnp.concatenate(x, axis=1)) * kin[part]
        x = times_left(zi[...], x)
        for z in range(ZL):
            for i in range(SL):
                back[part, pl.ds(SL * z + i, NZ, stride=SL * ZL), :] = x[z * NZ : (z + 1) * NZ, i * N : (i + 1) * N]
        by_parity(functools.partial(z_back, part))

    for part in range(2):
        by_parity(functools.partial(b_wait, part))
        x = ret[part]
        corr = corr + folded(sent[part] * x)
        square = square + folded(x * (x + 2.0 * wave[part]))
        if part == 1:
            row = jnp.zeros((1, N), F32)
            for i, value in enumerate((norm, corr, square)):
                total = jnp.sum(jnp.sum(value, axis=0, keepdims=True), axis=1, keepdims=True)
                row = jnp.where(lane == 16 * i + my, total, row)
            row1[...] = row
            tot1[mz] = row

            for d, _ in z_peers:
                pltpu.make_async_remote_copy(
                    row1, tot1.at[mz], r_send.at[0], r_recv.at[0], device_id=(my, d), device_id_type=MESH
                ).start()

        x = [ret[part, z] for z in range(ZL)]
        guest = times_right(jnp.concatenate([jnp.where(holds, 0.0, a[:FOLD]) for a in x], axis=0), gi[...])
        live = [b for a in x for b in (jnp.where(holds, a[:FOLD], 0.0), a[FOLD:])]
        live = times_right(jnp.concatenate(live, axis=0), ri[...])
        x = [
            jnp.concatenate([live[z * LIVE : (z + 1) * LIVE], guest[z * FOLD : (z + 1) * FOLD]], axis=0)
            for z in range(ZL)
        ]
        x = times_left(li[...], jnp.concatenate(x, axis=1))
        for z in range(ZL):
            app[part, z] = x[:, z * N : (z + 1) * N] + pot[z] * planes[part, z]

        for j in y_peers:
            pltpu.make_async_remote_copy(
                app.at[part, :, pl.ds(pl.multiple_of(j * YL, YL), YL), :], out.at[part, my],
                o_send.at[part], o_recv.at[part],
                device_id=(j, mz), device_id_type=MESH,
            ).start()
        out[part, my] = app[part, :, mine, :]

    drain(tot1.at[pl.ds(0, NZ - 1)], r_recv.at[0], "r0")
    row = jnp.sum(tot1[...], axis=0)
    row2[...] = row
    tot2[my] = row

    for j in y_peers:
        pltpu.make_async_remote_copy(
            row2, tot2.at[my], r_send.at[1], r_recv.at[1], device_id=(j, mz), device_id_type=MESH
        ).start()

    for part in range(2):
        by_parity(lambda odd, part=part: drain(slot_rows(part, odd), z_send.at[part]))
        by_parity(lambda odd, part=part: drain(z_rows(part, odd), b_send.at[part]))
        drain(app.at[part, :, others, :], o_send.at[part])
        drain(out.at[part, pl.ds(0, NY - 1)], o_recv.at[part], f"o{part}")
    drain(pot.at[:, others, :], y_send.at[len(CHUNKS)])
    for c, (part, z, nz) in enumerate(CHUNKS):
        drain(planes.at[part, pl.ds(z, nz), others, :], y_send.at[c])
    drain(tot1.at[pl.ds(0, NZ - 1)], r_send.at[0])

    keep = jnp.zeros((1, NB), F32)
    for b in range(NB):
        keep = jnp.where(lane[:, :NB] == b, 1.0 - locked[b].astype(F32), keep)
    drain(tot2.at[pl.ds(0, NY - 1)], r_recv.at[1], "r1")
    row = jnp.sum(tot2[...], axis=0)
    norm = row[:, 0:NB]
    corr = row[:, 16 : 16 + NB]
    square = row[:, 32 : 32 + NB]
    rayleigh = corr / norm
    ray_ref[...] = rayleigh.reshape(NB)
    res_ref[...] = (jnp.sqrt((square - rayleigh * corr) / norm) * keep).reshape(NB)
    drain(tot2.at[pl.ds(0, NY - 1)], r_send.at[1])


def write_out(applied, rayleigh, residual, *rest):
    sources, sem = (applied, rayleigh, residual), rest[3]
    copies = [pltpu.make_async_copy(a, b, sem.at[i]) for i, (a, b) in enumerate(zip(sources, rest[:3], strict=True))]
    for copy in copies:
        copy.start()
    for copy in copies:
        copy.wait()


def body(wavefunctions, potential, cutoff_sq, locked_mask):
    consts = [jnp.asarray(t) for t in tables()]
    hbm = pl.BlockSpec(memory_space=pltpu.HBM)
    vmem = pl.BlockSpec(memory_space=pltpu.VMEM)
    dma = pltpu.SemaphoreType.DMA
    applied, rayleigh, residual = pl.pallas_call(
        kernel,
        out_shape=(
            pltpu.VMEM((2, NB, ZL, YL, N), F32),
            pltpu.VMEM((NB,), F32),
            pltpu.VMEM((NB,), F32),
        ),
        in_specs=[hbm] * 12,
        out_specs=(vmem, vmem, vmem),
        scratch_shapes=[
            pltpu.VMEM((2, NB, ZL, YL, N), F32),
            pltpu.VMEM((ZL, YL, N), F32),
            pltpu.SMEM((1,), jnp.int32),
            pltpu.SMEM((NB,), jnp.int32),
            *[pltpu.VMEM(t.shape, BF16) for t in consts],
            pltpu.VMEM((2, ZL, N, N), F32),
            pltpu.VMEM((ZL, N, N), F32),
            pltpu.VMEM((2, ZL, LIVE, N), F32),
            pltpu.VMEM((2, NZ * ZL * SL, N), F32),
            pltpu.VMEM((2, NZ * ZL * SL, N), F32),
            pltpu.VMEM((2, ZL, LIVE, N), F32),
            pltpu.VMEM((2, ZL, LIVE, N), F32),
            pltpu.VMEM((2, ZL, N, N), F32),
            pltpu.VMEM((2, N, SL * N), F32),
            pltpu.VMEM((1, N), F32),
            pltpu.VMEM((1, N), F32),
            pltpu.VMEM((NZ, 1, N), F32),
            pltpu.VMEM((NY, 1, N), F32),
            dma((12,)),
            dma((len(CHUNKS) + 1,)), dma((len(CHUNKS) + 1,)), dma((2,)), dma((2,)), dma((2,)), dma((2,)),
            dma((2,)), dma((2,)), dma((len(CHUNKS) + 2,)), dma((2,)), dma((2,)),
            pltpu.SemaphoreType.REGULAR((len(ROUNDS),)),
        ],
        compiler_params=pltpu.CompilerParams(collective_id=0, has_side_effects=True),
    )(wavefunctions, potential, cutoff_sq, locked_mask, *consts)
    return pl.pallas_call(
        write_out,
        out_shape=(
            jax.ShapeDtypeStruct((2, NB, ZL, YL, N), F32),
            jax.ShapeDtypeStruct((NB,), F32),
            jax.ShapeDtypeStruct((NB,), F32),
        ),
        in_specs=[vmem] * 3,
        out_specs=(hbm,) * 3,
        scratch_shapes=[dma((3,))],
    )(*[pltpu.with_memory_space_constraint(a, pltpu.VMEM) for a in (applied, rayleigh, residual)])


def solution(mesh):
    placed = (P(None, None, "pz", "py", None), P("pz", "py", None), P(), P())
    return jax.shard_map(
        body,
        mesh=mesh,
        in_specs=placed,
        out_specs=(P(None, None, "pz", "py", None), P(), P()),
        check_vma=False,
    )
```

```python
import functools
import itertools
import math

import jax
import jax.numpy as jnp
import numpy as np
from jax import lax
from jax.experimental import pallas as pl
from jax.experimental.pallas import tpu as pltpu
from jax.sharding import PartitionSpec as P

N = 128
NB = 8
NY = 8
NZ = 32
ZL = N // NZ
YL = N // NY
ENTRY = ((0, 2), (0, 6), (2, 0), (1, 1), (1, 7), (3, 1), (3, 7), (1, 0), (3, 0), (0, 1), (0, 7))
ROUNDS = (((0, 2), (0, 6), (2, 0)), ((0, 2), (0, 6)))
SENT_IN = ((0, 1, 2, 3), (), ())
BACKS = ((0, 0, 4), (1, 0, 4))
TOLD = 64
SL = N // NZ
CHUNKS = ((0, 0, 1), (0, 1, 1), (0, 2, 2), (1, 0, 4))
LIVE = 112
FOLD = N - LIVE
HOST = 48
SPHERE = N * N // 4
MESH = pl.DeviceIdType.MESH
F32 = jnp.float32
BF16 = jnp.bfloat16


def basis():
    n = np.arange(N)
    rows = []
    for m in range(N):
        k = (m + 1) // 2
        angle = 2.0 * np.pi * ((k * n) % N) / N
        row = np.cos(angle) if (m % 2 == 1 or m == 0) else np.sin(angle)
        scale = 1.0 / N if k in (0, N // 2) else 2.0 / N
        rows.append(np.sqrt(scale) * row)
    return np.stack(rows)


def high_low(table):
    high = table.astype(BF16)
    low = (table - high.astype(np.float64)).astype(BF16)
    return high, low


def row_order():
    hosts = [2 * k - 1 + c for k in range(HOST, HOST + FOLD // 2) for c in range(2)]
    guests = [2 * (111 - k) - 1 + c for k in range(HOST, HOST + FOLD // 2) for c in range(2)]
    plain = [m for m in range(N) if m not in hosts and m not in guests]
    for host, guest in zip(hosts, guests, strict=True):
        width = [sum(((m + 1) // 2) ** 2 + ((r + 1) // 2) ** 2 <= SPHERE for m in range(N)) for r in (host, guest)]
        assert sum(width) <= N
    return hosts + plain + guests


def tables():
    f = basis()
    fh, fl = high_low(f)
    ph, pl_ = fh[row_order()], fl[row_order()]
    right_fwd = np.block([[fh.T, fl.T], [fh.T, fl.T]])
    right_inv = np.block([[fh, fl], [fh, fl]])
    guest_fwd = np.block([[fh[::-1].T, fl[::-1].T], [fh[::-1].T, fl[::-1].T]])
    guest_inv = np.block([[fh[::-1], fl[::-1]], [fh[::-1], fl[::-1]]])
    left_fwd = np.block([[ph, ph], [pl_, pl_]])
    left_inv = np.block([[ph.T, ph.T], [pl_.T, pl_.T]])
    zh, zl = (t.reshape(N, NZ, ZL).swapaxes(1, 2).reshape(N, N) for t in (fh, fl))
    z_fwd = np.block([[zh, zh], [zl, zl]])
    z_inv = np.block([[zh.T, zh.T], [zl.T, zl.T]])
    return [right_fwd, guest_fwd, left_fwd, right_inv, guest_inv, left_inv, z_fwd, z_inv]


def split(x):
    high = x.astype(BF16)
    low = (x - high.astype(F32)).astype(BF16)
    return high, low


def dot(a, b):
    return jnp.dot(a, b, preferred_element_type=F32)


def times_right(x, table):
    high, low = split(x)
    both = dot(jnp.concatenate([high, low], axis=1), table)
    return both[:, :N] + both[:, N:]


def times_left(table, x):
    high, low = split(x)
    both = dot(table, jnp.concatenate([high, low], axis=0))
    return both[:N] + both[N:]


def kernel(
    u_hbm, v_hbm, cutoff_hbm, locked_hbm, rf_hbm, gf_hbm, lf_hbm, ri_hbm, gi_hbm, li_hbm, zf_hbm, zi_hbm,
    out, ray_ref, res_ref,
    u_in, v_in, cutoff, locked, rf, gf, lf, ri, gi, li, zf, zi,
    planes, pot, sent, got, back, ret, wave, app, kin, row1, sums,
    in_sem, y_send, y_recv, z_send, z_recv, b_send, b_recv, o_send, o_recv, own, r_send, r_recv, r_own, rounds,
):
    my = lax.axis_index("py")
    mz = lax.axis_index("pz")

    y_chip = [lax.rem(my // 2 + d, 4) * 2 for d in range(4)]
    y_core = [lax.rem(my + d, 2) for d in range(2)]
    y_peers = [y_chip[d] + y_core[c] for d in (2, 1, 3, 0) for c in (0, 1) if d or c]
    z_x = [lax.rem(mz // 8 + d, 4) * 8 for d in range(4)]
    z_z = [lax.rem(mz + d, 8) for d in range(8)]
    z_peers = [(z_x[d] + z_z[e], e % 2) for d in (2, 1, 3, 0) for e in (4, 3, 5, 2, 6, 1, 7, 0) if d or e]

    def load(i, source, target):
        copy = pltpu.make_async_copy(source, target, in_sem.at[i])
        copy.start()
        return copy

    first = [load(0, u_hbm, u_in), load(1, v_hbm, v_in)]
    barrier = pltpu.get_barrier_semaphore()

    def greet(sem, offsets):
        for d, e in offsets:
            pl.semaphore_signal(sem, inc=1, device_id=(my, z_x[d] + z_z[e]), device_id_type=MESH)

    greet(barrier, ENTRY)
    for j in y_peers:
        pl.semaphore_signal(barrier, inc=1, device_id=(j, mz), device_id_type=MESH)

    later = [(lf_hbm, lf), (rf_hbm, rf), (gf_hbm, gf), (cutoff_hbm, cutoff), (locked_hbm, locked), (zf_hbm, zf), (zi_hbm, zi), (ri_hbm, ri), (gi_hbm, gi), (li_hbm, li)]
    later = [load(i + 2, a, b) for i, (a, b) in enumerate(later)]
    for copy in first:
        copy.wait()
    with jax.named_scope("barrier"):
        pl.semaphore_wait(barrier, len(ENTRY) + NY - 1)

    def drain(ref, sem, name="end"):
        with jax.named_scope(name):
            pltpu.make_async_copy(ref, ref, sem).wait()

    mine = pl.ds(pl.multiple_of(my * YL, YL), YL)
    def y_out(c):
        part, z, nz = CHUNKS[c]
        for j in y_peers:
            pltpu.make_async_remote_copy(
                u_in.at[part, j, pl.ds(z, nz)], planes.at[part, pl.ds(z, nz), mine, :], y_send.at[c], y_recv.at[c],
                device_id=(j, mz), device_id_type=MESH,
            ).start()

    for r, offsets in enumerate(ROUNDS):
        if r:
            with jax.named_scope(f"round{r}"):
                pl.semaphore_wait(rounds.at[r - 1], len(ROUNDS[r - 1]))
        greet(rounds.at[r], offsets)
        for c in SENT_IN[r]:
            y_out(c)
    with jax.named_scope("roundlast"):
        pl.semaphore_wait(rounds.at[len(ROUNDS) - 1], len(ROUNDS[-1]))
    for c in SENT_IN[len(ROUNDS)]:
        y_out(c)
    for j in y_peers:
        pltpu.make_async_remote_copy(
            v_in, pot.at[:, mine, :], y_send.at[len(CHUNKS)], y_recv.at[len(CHUNKS)],
            device_id=(j, mz), device_id_type=MESH,
        ).start()
    planes[:, :, mine, :] = u_in[:, my]
    pot[:, mine, :] = v_in[...]
    for copy in later:
        copy.wait()

    def first_slot(d, odd, part):
        return 7 * (d // 2) + (4 - part) * odd

    def slots(odd, part):
        return 4 - (odd + part) % 2

    lane = lax.broadcasted_iota(jnp.int32, (1, N), 1)
    mine_row = pl.ds(mz * NY + my, 1)
    up = (lane + 1) // 2
    down = (N - lane) // 2
    others = pl.ds(0, (NY - 1) * YL)
    own_row = HOST + lax.broadcasted_iota(jnp.int32, (FOLD, N), 0) // 2
    own_kx = (lax.broadcasted_iota(jnp.int32, (FOLD, N), 1) + 1) // 2
    holds = own_row * own_row + own_kx * own_kx <= SPHERE

    def plane_transform(field, target, part, first, count):
        x = times_left(lf[...], jnp.concatenate([field[z] for z in range(count)], axis=1))
        x = [x[:, z * N : (z + 1) * N] for z in range(count)]
        guest = times_right(jnp.concatenate([a[LIVE:] for a in x], axis=0), gf[...])
        live = times_right(jnp.concatenate([a[:LIVE] for a in x], axis=0), rf[...])
        for z in range(count):
            a = live[z * LIVE : (z + 1) * LIVE]
            target[part, first + z, :FOLD, :] = jnp.where(holds, a[:FOLD], guest[z * FOLD : (z + 1) * FOLD])
            target[part, first + z, FOLD:, :] = a[FOLD:]

    def by_parity(act):
        for odd in range(2):
            pl.when(lax.rem(mz, 2) == odd)(functools.partial(act, odd))

    got_view = got.reshape(2, NZ, ZL, SL, N)
    back_view = back.reshape(2, NZ, ZL, SL, N)

    def z_out(part, first, count, c, odd):
        def copy_of(d, o):
            n = slots(o, part)
            return (
                sent.at[part, pl.ds(first, count), pl.ds(first_slot(d, o, part), n), :],
                got_view.at[part, mz, pl.ds(first, count), pl.ds(0, n), :],
            )

        for d, e in z_peers:
            a, b = copy_of(d, (odd + e) % 2)
            pltpu.make_async_remote_copy(
                a, b, z_send.at[part], z_recv.at[part], device_id=(my, d), device_id_type=MESH
            ).start()
        pltpu.make_async_copy(*copy_of(mz, odd), own.at[c]).start()

    def z_back(c, odd):
        part, first, count = BACKS[c]
        n = slots(odd, part)
        target = ret.at[part, pl.ds(first, count), pl.ds(first_slot(mz, odd, part), n), :]
        for d, _ in z_peers:
            pltpu.make_async_remote_copy(
                back_view.at[part, d, pl.ds(first, count), pl.ds(0, n), :], target, b_send.at[c], b_recv.at[c],
                device_id=(my, d), device_id_type=MESH,
            ).start()
        pltpu.make_async_copy(
            back_view.at[part, mz, pl.ds(first, count), pl.ds(0, n), :], target, own.at[len(CHUNKS) + c]
        ).start()

    def z_rows(part, odd, count=ZL):
        return got_view.at[part, pl.ds(0, NZ - 1), pl.ds(0, count), pl.ds(0, slots(odd, part)), :]

    def slot_rows(part, odd, count=ZL):
        return ret.at[part, pl.ds(0, count), pl.ds(0, LIVE - slots(odd, part)), :]

    def own_wait(part, count, c, odd):
        a = ret.at[part, pl.ds(0, count), pl.ds(0, slots(odd, part)), :]
        pltpu.make_async_copy(a, a, own.at[c]).wait()

    def z_wait(part, odd):
        drain(z_rows(part, odd), z_recv.at[part], f"z{part}")
        for c, (p, _, count) in enumerate(CHUNKS):
            if p == part:
                own_wait(part, count, c, odd)

    def b_wait(c, odd):
        part, _, count = BACKS[c]
        drain(slot_rows(part, odd, count), b_recv.at[c], f"b{c}")
        own_wait(part, count, len(CHUNKS) + c, odd)

    for c, (part, z, nz) in enumerate(CHUNKS):
        drain(planes.at[part, pl.ds(z, nz), others, :], y_recv.at[c], f"y{c}")
        plane_transform(planes[part, z : z + nz], sent, part, z, nz)
        by_parity(functools.partial(z_out, part, z, nz, c))

    for part in range(2):
        start = first_slot(mz, lax.rem(mz, 2), part)
        for i in range(SL):
            slot = start + i
            host = slot < FOLD
            ky = jnp.where(host, HOST + slot // 2, jnp.where(slot == LIVE - 1, N // 2, (slot - FOLD + 1) // 2))
            s = ky * ky + up * up
            s = jnp.where(s > jnp.where(host, SPHERE, 4 * SPHERE), (111 - ky) * (111 - ky) + down * down, s)
            kz = (lax.broadcasted_iota(jnp.int32, (N, N), 0) + 1) // 2
            s = s + kz * kz
            kin[part, :, i * N : (i + 1) * N] = jnp.where(
                s <= cutoff[0], 0.5 * (math.pi / N) ** 2 * s.astype(F32), 0.0
            )

    def folded(x):
        return jnp.sum(x.reshape(-1, 8, N), axis=0)

    drain(pot.at[:, others, :], y_recv.at[len(CHUNKS)], "pot")
    norm = corr = square = jnp.zeros((8, N), F32)
    for part in range(2):
        field = planes[part]
        local = pot[...] * field
        norm = norm + folded(field * field)
        corr = corr + folded(field * local)
        square = square + folded(local * local)
        plane_transform(local, wave, part, 0, ZL)

    for part in range(2):
        by_parity(functools.partial(z_wait, part))
        x = [
            jnp.concatenate([got[part, pl.ds(SL * z + i, NZ, stride=SL * ZL), :] for z in range(ZL)], axis=0)
            for i in range(SL)
        ]
        x = times_left(zf[...], jnp.concatenate(x, axis=1)) * kin[part]
        x = times_left(zi[...], x)
        for z in range(ZL):
            for i in range(SL):
                back[part, pl.ds(SL * z + i, NZ, stride=SL * ZL), :] = x[z * NZ : (z + 1) * NZ, i * N : (i + 1) * N]
        for c, back_chunk in enumerate(BACKS):
            if back_chunk[0] == part:
                by_parity(functools.partial(z_back, c))

    def tell(offsets):
        for a, b, d, e in offsets:
            pltpu.make_async_remote_copy(
                row1, sums.at[mine_row, :], r_send.at[0], r_recv.at[0],
                device_id=(y_chip[a] + y_core[b], z_x[d] + z_z[e]), device_id_type=MESH,
            ).start()

    everyone = sorted(
        [p for p in itertools.product(range(4), range(2), range(4), range(8)) if any(p)],
        key=lambda p: -4 * (min(p[0], 4 - p[0]) + min(p[2], 4 - p[2]) + min(p[3], 8 - p[3])) - p[1],
    )
    for c, (part, first, count) in enumerate(BACKS):
        by_parity(functools.partial(b_wait, c))
        some = pl.ds(first, count)
        x = ret[part, some]
        corr = corr + folded(sent[part, some] * x)
        square = square + folded(x * (x + 2.0 * wave[part, some]))
        last = c == len(BACKS) - 1
        if last:
            row = jnp.zeros((1, N), F32)
            for i, value in enumerate((norm, corr, square)):
                total = jnp.sum(jnp.sum(value, axis=0, keepdims=True), axis=1, keepdims=True)
                row = jnp.where(lane == i, total, row)
            row1[...] = row
            tell(everyone[:TOLD])
        x = [ret[part, first + z] for z in range(count)]
        guest = times_right(jnp.concatenate([jnp.where(holds, 0.0, a[:FOLD]) for a in x], axis=0), gi[...])
        live = [b for a in x for b in (jnp.where(holds, a[:FOLD], 0.0), a[FOLD:])]
        live = times_right(jnp.concatenate(live, axis=0), ri[...])
        x = [
            jnp.concatenate([live[z * LIVE : (z + 1) * LIVE], guest[z * FOLD : (z + 1) * FOLD]], axis=0)
            for z in range(count)
        ]
        x = times_left(li[...], jnp.concatenate(x, axis=1))
        for z in range(count):
            app[part, first + z] = x[:, z * N : (z + 1) * N] + pot[first + z] * planes[part, first + z]
        for j in y_peers:
            pltpu.make_async_remote_copy(
                app.at[part, some, pl.ds(pl.multiple_of(j * YL, YL), YL), :], out.at[part, my, some],
                o_send.at[c], o_recv.at[c],
                device_id=(j, mz), device_id_type=MESH,
            ).start()
        if last:
            tell(everyone[TOLD:])
            pltpu.make_async_copy(row1, sums.at[mine_row, :], r_own).start()
        out[part, my, some] = app[part, some, mine, :]

    for part in range(2):
        by_parity(lambda odd, part=part: drain(slot_rows(part, odd), z_send.at[part]))
    for c, (part, first, count) in enumerate(BACKS):
        by_parity(lambda odd, c=c, part=part, count=count: drain(z_rows(part, odd, count), b_send.at[c]))
        drain(app.at[part, pl.ds(first, count), others, :], o_send.at[c], f"s{c}")
        drain(out.at[part, pl.ds(0, NY - 1), pl.ds(first, count)], o_recv.at[c], f"o{c}")
    drain(pot.at[:, others, :], y_send.at[len(CHUNKS)])
    for c, (part, z, nz) in enumerate(CHUNKS):
        drain(planes.at[part, pl.ds(z, nz), others, :], y_send.at[c])

    told = sums.at[pl.ds(0, NY * NZ - 1), :]
    drain(told, r_send.at[0])
    pltpu.make_async_copy(row1, sums.at[mine_row, :], r_own).wait()
    band = lax.broadcasted_iota(jnp.int32, (NB, NB), 0)
    same = band == lax.broadcasted_iota(jnp.int32, (NB, NB), 1)
    keep = jnp.zeros((NB, NB), F32)
    for b in range(NB):
        keep = jnp.where(band == b, 1.0 - locked[b].astype(F32), keep)
    drain(told, r_recv.at[0], "r0")
    total = jnp.sum(sums[...].reshape(NZ, NY, N), axis=0)
    norm, corr, square = (jnp.broadcast_to(total[:, i : i + 1], (NB, NB)) for i in range(3))
    rayleigh = corr / norm
    residual = jnp.sqrt((square - rayleigh * corr) / norm) * keep
    ray_ref[...] = jnp.sum(jnp.where(same, rayleigh, 0.0), axis=0)
    res_ref[...] = jnp.sum(jnp.where(same, residual, 0.0), axis=0)


def write_out(applied, rayleigh, residual, *rest):
    sources, sem = (applied, rayleigh, residual), rest[3]
    copies = [pltpu.make_async_copy(a, b, sem.at[i]) for i, (a, b) in enumerate(zip(sources, rest[:3], strict=True))]
    for copy in copies:
        copy.start()
    for copy in copies:
        copy.wait()


def body(wavefunctions, potential, cutoff_sq, locked_mask):
    consts = [jnp.asarray(t) for t in tables()]
    hbm = pl.BlockSpec(memory_space=pltpu.HBM)
    vmem = pl.BlockSpec(memory_space=pltpu.VMEM)
    dma = pltpu.SemaphoreType.DMA
    applied, rayleigh, residual = pl.pallas_call(
        kernel,
        out_shape=(
            pltpu.VMEM((2, NB, ZL, YL, N), F32),
            pltpu.VMEM((NB,), F32),
            pltpu.VMEM((NB,), F32),
        ),
        in_specs=[hbm] * 12,
        out_specs=(vmem, vmem, vmem),
        scratch_shapes=[
            pltpu.VMEM((2, NB, ZL, YL, N), F32),
            pltpu.VMEM((ZL, YL, N), F32),
            pltpu.SMEM((1,), jnp.int32),
            pltpu.SMEM((NB,), jnp.int32),
            *[pltpu.VMEM(t.shape, BF16) for t in consts],
            pltpu.VMEM((2, ZL, N, N), F32),
            pltpu.VMEM((ZL, N, N), F32),
            pltpu.VMEM((2, ZL, LIVE, N), F32),
            pltpu.VMEM((2, NZ * ZL * SL, N), F32),
            pltpu.VMEM((2, NZ * ZL * SL, N), F32),
            pltpu.VMEM((2, ZL, LIVE, N), F32),
            pltpu.VMEM((2, ZL, LIVE, N), F32),
            pltpu.VMEM((2, ZL, N, N), F32),
            pltpu.VMEM((2, N, SL * N), F32),
            pltpu.VMEM((1, N), F32),
            pltpu.VMEM((NZ * NY, N), F32),
            dma((12,)),
            dma((len(CHUNKS) + 1,)), dma((len(CHUNKS) + 1,)), dma((2,)), dma((2,)), dma((len(BACKS),)), dma((len(BACKS),)),
            dma((len(BACKS),)), dma((len(BACKS),)), dma((len(CHUNKS) + len(BACKS),)), dma((1,)), dma((1,)), dma(()),
            pltpu.SemaphoreType.REGULAR((len(ROUNDS),)),
        ],
        compiler_params=pltpu.CompilerParams(collective_id=0, has_side_effects=True),
    )(wavefunctions, potential, cutoff_sq, locked_mask, *consts)
    return pl.pallas_call(
        write_out,
        out_shape=(
            jax.ShapeDtypeStruct((2, NB, ZL, YL, N), F32),
            jax.ShapeDtypeStruct((NB,), F32),
            jax.ShapeDtypeStruct((NB,), F32),
        ),
        in_specs=[vmem] * 3,
        out_specs=(hbm,) * 3,
        scratch_shapes=[dma((3,))],
    )(*[pltpu.with_memory_space_constraint(a, pltpu.VMEM) for a in (applied, rayleigh, residual)])


def solution(mesh):
    placed = (P(None, None, "pz", "py", None), P("pz", "py", None), P(), P())
    return jax.shard_map(
        body,
        mesh=mesh,
        in_specs=placed,
        out_specs=(P(None, None, "pz", "py", None), P(), P()),
        check_vma=False,
    )
```

```python
import functools
import itertools
import math

import jax
import jax.numpy as jnp
import numpy as np
from jax import lax
from jax.experimental import pallas as pl
from jax.experimental.pallas import tpu as pltpu
from jax.sharding import PartitionSpec as P

N = 128
NB = 8
NY = 8
NZ = 32
ZL = N // NZ
YL = N // NY
ENTRY = ((0, 2), (0, 6), (2, 0), (1, 1), (1, 7), (3, 1), (3, 7), (1, 0), (3, 0), (0, 1), (0, 7))
ROUNDS = (((0, 2), (0, 6), (2, 0)), ((0, 2), (0, 6)))
SENT_IN = ((0, 1, 2, 3), (), ())
BACKS = ((0, 0, 4), (1, 0, 4))
TOLD = 64
SL = N // NZ
CHUNKS = ((0, 0, 1), (0, 1, 1), (0, 2, 2), (1, 0, 4))
LIVE = 112
FOLD = N - LIVE
HOST = 48
SPHERE = N * N // 4
MESH = pl.DeviceIdType.MESH
F32 = jnp.float32
BF16 = jnp.bfloat16


def basis():
    n = np.arange(N)
    rows = []
    for m in range(N):
        k = (m + 1) // 2
        angle = 2.0 * np.pi * ((k * n) % N) / N
        row = np.cos(angle) if (m % 2 == 1 or m == 0) else np.sin(angle)
        scale = 1.0 / N if k in (0, N // 2) else 2.0 / N
        rows.append(np.sqrt(scale) * row)
    return np.stack(rows)


def high_low(table):
    high = table.astype(BF16)
    low = (table - high.astype(np.float64)).astype(BF16)
    return high, low


def row_order():
    hosts = [2 * k - 1 + c for k in range(HOST, HOST + FOLD // 2) for c in range(2)]
    guests = [2 * (111 - k) - 1 + c for k in range(HOST, HOST + FOLD // 2) for c in range(2)]
    plain = [m for m in range(N) if m not in hosts and m not in guests]
    for host, guest in zip(hosts, guests, strict=True):
        width = [sum(((m + 1) // 2) ** 2 + ((r + 1) // 2) ** 2 <= SPHERE for m in range(N)) for r in (host, guest)]
        assert sum(width) <= N
    return hosts + plain + guests


def tables():
    f = basis()
    fh, fl = high_low(f)
    ph, pl_ = fh[row_order()], fl[row_order()]
    right_fwd = np.block([[fh.T, fl.T], [fh.T, fl.T]])
    right_inv = np.block([[fh, fl], [fh, fl]])
    guest_fwd = np.block([[fh[::-1].T, fl[::-1].T], [fh[::-1].T, fl[::-1].T]])
    guest_inv = np.block([[fh[::-1], fl[::-1]], [fh[::-1], fl[::-1]]])
    left_fwd = np.block([[ph, ph], [pl_, pl_]])
    left_inv = np.block([[ph.T, ph.T], [pl_.T, pl_.T]])
    zh, zl = (t.reshape(N, NZ, ZL).swapaxes(1, 2).reshape(N, N) for t in (fh, fl))
    z_fwd = np.block([[zh, zh], [zl, zl]])
    z_inv = np.block([[zh.T, zh.T], [zl.T, zl.T]])
    return [right_fwd, guest_fwd, left_fwd, right_inv, guest_inv, left_inv, z_fwd, z_inv]


def split(x):
    high = x.astype(BF16)
    low = (x - high.astype(F32)).astype(BF16)
    return high, low


def dot(a, b):
    return jnp.dot(a, b, preferred_element_type=F32)


def times_right(x, table):
    high, low = split(x)
    both = dot(jnp.concatenate([high, low], axis=1), table)
    return both[:, :N] + both[:, N:]


def times_left(table, x):
    high, low = split(x)
    both = dot(table, jnp.concatenate([high, low], axis=0))
    return both[:N] + both[N:]


def kernel(
    u_hbm, v_hbm, cutoff_hbm, locked_hbm, rf_hbm, gf_hbm, lf_hbm, ri_hbm, gi_hbm, li_hbm, zf_hbm, zi_hbm,
    out, sums, keep_ref,
    u_in, v_in, cutoff, locked, rf, gf, lf, ri, gi, li, zf, zi,
    planes, pot, sent, got, back, ret, wave, app, kin, row1,
    in_sem, y_send, y_recv, z_send, z_recv, b_send, b_recv, o_send, o_recv, own, r_send, r_recv, r_own, rounds,
):
    my = lax.axis_index("py")
    mz = lax.axis_index("pz")

    y_chip = [lax.rem(my // 2 + d, 4) * 2 for d in range(4)]
    y_core = [lax.rem(my + d, 2) for d in range(2)]
    y_peers = [y_chip[d] + y_core[c] for d in (2, 1, 3, 0) for c in (0, 1) if d or c]
    z_x = [lax.rem(mz // 8 + d, 4) * 8 for d in range(4)]
    z_z = [lax.rem(mz + d, 8) for d in range(8)]
    by_hops = sorted(
        [p for p in itertools.product((2, 1, 3, 0), (4, 3, 5, 2, 6, 1, 7, 0)) if any(p)],
        key=lambda p: -min(p[0], 4 - p[0]) - min(p[1], 8 - p[1]),
    )
    z_peers = [(z_x[d] + z_z[e], e % 2) for d, e in by_hops]

    def load(i, source, target):
        copy = pltpu.make_async_copy(source, target, in_sem.at[i])
        copy.start()
        return copy

    first = [load(0, u_hbm, u_in), load(1, v_hbm, v_in)]
    barrier = pltpu.get_barrier_semaphore()

    def greet(sem, offsets):
        for d, e in offsets:
            pl.semaphore_signal(sem, inc=1, device_id=(my, z_x[d] + z_z[e]), device_id_type=MESH)

    greet(barrier, ENTRY)
    for j in y_peers:
        pl.semaphore_signal(barrier, inc=1, device_id=(j, mz), device_id_type=MESH)

    later = [(lf_hbm, lf), (rf_hbm, rf), (gf_hbm, gf), (cutoff_hbm, cutoff), (locked_hbm, locked), (zf_hbm, zf), (zi_hbm, zi), (ri_hbm, ri), (gi_hbm, gi), (li_hbm, li)]
    later = [load(i + 2, a, b) for i, (a, b) in enumerate(later)]
    for copy in first:
        copy.wait()
    with jax.named_scope("barrier"):
        pl.semaphore_wait(barrier, len(ENTRY) + NY - 1)

    def drain(ref, sem, name="end"):
        with jax.named_scope(name):
            pltpu.make_async_copy(ref, ref, sem).wait()

    mine = pl.ds(pl.multiple_of(my * YL, YL), YL)
    def y_out(c):
        part, z, nz = CHUNKS[c]
        for j in y_peers:
            pltpu.make_async_remote_copy(
                u_in.at[part, j, pl.ds(z, nz)], planes.at[part, pl.ds(z, nz), mine, :], y_send.at[c], y_recv.at[c],
                device_id=(j, mz), device_id_type=MESH,
            ).start()

    for r, offsets in enumerate(ROUNDS):
        if r:
            with jax.named_scope(f"round{r}"):
                pl.semaphore_wait(rounds.at[r - 1], len(ROUNDS[r - 1]))
        greet(rounds.at[r], offsets)
        for c in SENT_IN[r]:
            y_out(c)
    with jax.named_scope("roundlast"):
        pl.semaphore_wait(rounds.at[len(ROUNDS) - 1], len(ROUNDS[-1]))
    for c in SENT_IN[len(ROUNDS)]:
        y_out(c)
    for j in y_peers:
        pltpu.make_async_remote_copy(
            v_in, pot.at[:, mine, :], y_send.at[len(CHUNKS)], y_recv.at[len(CHUNKS)],
            device_id=(j, mz), device_id_type=MESH,
        ).start()
    planes[:, :, mine, :] = u_in[:, my]
    pot[:, mine, :] = v_in[...]
    for copy in later:
        copy.wait()

    def first_slot(d, odd, part):
        return 7 * (d // 2) + (4 - part) * odd

    def slots(odd, part):
        return 4 - (odd + part) % 2

    lane = lax.broadcasted_iota(jnp.int32, (1, N), 1)
    mine_row = pl.ds(mz * NY + my, 1)
    up = (lane + 1) // 2
    down = (N - lane) // 2
    others = pl.ds(0, (NY - 1) * YL)
    own_row = HOST + lax.broadcasted_iota(jnp.int32, (FOLD, N), 0) // 2
    own_kx = (lax.broadcasted_iota(jnp.int32, (FOLD, N), 1) + 1) // 2
    holds = own_row * own_row + own_kx * own_kx <= SPHERE

    def plane_transform(field, target, part, first, count):
        x = times_left(lf[...], jnp.concatenate([field[z] for z in range(count)], axis=1))
        x = [x[:, z * N : (z + 1) * N] for z in range(count)]
        guest = times_right(jnp.concatenate([a[LIVE:] for a in x], axis=0), gf[...])
        live = times_right(jnp.concatenate([a[:LIVE] for a in x], axis=0), rf[...])
        for z in range(count):
            a = live[z * LIVE : (z + 1) * LIVE]
            target[part, first + z, :FOLD, :] = jnp.where(holds, a[:FOLD], guest[z * FOLD : (z + 1) * FOLD])
            target[part, first + z, FOLD:, :] = a[FOLD:]

    def by_parity(act):
        for odd in range(2):
            pl.when(lax.rem(mz, 2) == odd)(functools.partial(act, odd))

    got_view = got.reshape(2, NZ, ZL, SL, N)
    back_view = back.reshape(2, NZ, ZL, SL, N)

    def z_out(part, first, count, c, odd):
        def copy_of(d, o):
            n = slots(o, part)
            return (
                sent.at[part, pl.ds(first, count), pl.ds(first_slot(d, o, part), n), :],
                got_view.at[part, mz, pl.ds(first, count), pl.ds(0, n), :],
            )

        for d, e in z_peers:
            a, b = copy_of(d, (odd + e) % 2)
            pltpu.make_async_remote_copy(
                a, b, z_send.at[part], z_recv.at[part], device_id=(my, d), device_id_type=MESH
            ).start()
        pltpu.make_async_copy(*copy_of(mz, odd), own.at[c]).start()

    def z_back(c, odd):
        part, first, count = BACKS[c]
        n = slots(odd, part)
        target = ret.at[part, pl.ds(first, count), pl.ds(first_slot(mz, odd, part), n), :]
        for d, _ in z_peers:
            pltpu.make_async_remote_copy(
                back_view.at[part, d, pl.ds(first, count), pl.ds(0, n), :], target, b_send.at[c], b_recv.at[c],
                device_id=(my, d), device_id_type=MESH,
            ).start()
        pltpu.make_async_copy(
            back_view.at[part, mz, pl.ds(first, count), pl.ds(0, n), :], target, own.at[len(CHUNKS) + c]
        ).start()

    def z_rows(part, odd, count=ZL):
        return got_view.at[part, pl.ds(0, NZ - 1), pl.ds(0, count), pl.ds(0, slots(odd, part)), :]

    def slot_rows(part, odd, count=ZL):
        return ret.at[part, pl.ds(0, count), pl.ds(0, LIVE - slots(odd, part)), :]

    def own_wait(part, count, c, odd):
        a = ret.at[part, pl.ds(0, count), pl.ds(0, slots(odd, part)), :]
        pltpu.make_async_copy(a, a, own.at[c]).wait()

    def z_wait(part, odd):
        drain(z_rows(part, odd), z_recv.at[part], f"z{part}")
        for c, (p, _, count) in enumerate(CHUNKS):
            if p == part:
                own_wait(part, count, c, odd)

    def b_wait(c, odd):
        part, _, count = BACKS[c]
        drain(slot_rows(part, odd, count), b_recv.at[c], f"b{c}")
        own_wait(part, count, len(CHUNKS) + c, odd)

    for c, (part, z, nz) in enumerate(CHUNKS):
        drain(planes.at[part, pl.ds(z, nz), others, :], y_recv.at[c], f"y{c}")
        plane_transform(planes[part, z : z + nz], sent, part, z, nz)
        by_parity(functools.partial(z_out, part, z, nz, c))

    for part in range(2):
        start = first_slot(mz, lax.rem(mz, 2), part)
        for i in range(SL):
            slot = start + i
            host = slot < FOLD
            ky = jnp.where(host, HOST + slot // 2, jnp.where(slot == LIVE - 1, N // 2, (slot - FOLD + 1) // 2))
            s = ky * ky + up * up
            s = jnp.where(s > jnp.where(host, SPHERE, 4 * SPHERE), (111 - ky) * (111 - ky) + down * down, s)
            kz = (lax.broadcasted_iota(jnp.int32, (N, N), 0) + 1) // 2
            s = s + kz * kz
            kin[part, :, i * N : (i + 1) * N] = jnp.where(
                s <= cutoff[0], 0.5 * (math.pi / N) ** 2 * s.astype(F32), 0.0
            )

    def folded(x):
        return jnp.sum(x.reshape(-1, 8, N), axis=0)

    drain(pot.at[:, others, :], y_recv.at[len(CHUNKS)], "pot")
    norm = corr = square = jnp.zeros((8, N), F32)
    for part in range(2):
        field = planes[part]
        local = pot[...] * field
        norm = norm + folded(field * field)
        corr = corr + folded(field * local)
        square = square + folded(local * local)
        plane_transform(local, wave, part, 0, ZL)

    for part in range(2):
        by_parity(functools.partial(z_wait, part))
        x = [
            jnp.concatenate([got[part, pl.ds(SL * z + i, NZ, stride=SL * ZL), :] for z in range(ZL)], axis=0)
            for i in range(SL)
        ]
        x = times_left(zf[...], jnp.concatenate(x, axis=1)) * kin[part]
        x = times_left(zi[...], x)
        for z in range(ZL):
            for i in range(SL):
                back[part, pl.ds(SL * z + i, NZ, stride=SL * ZL), :] = x[z * NZ : (z + 1) * NZ, i * N : (i + 1) * N]
        for c, back_chunk in enumerate(BACKS):
            if back_chunk[0] == part:
                by_parity(functools.partial(z_back, c))

    def tell(offsets):
        for a, b, d, e in offsets:
            pltpu.make_async_remote_copy(
                row1, sums.at[mine_row, :], r_send.at[0], r_recv.at[0],
                device_id=(y_chip[a] + y_core[b], z_x[d] + z_z[e]), device_id_type=MESH,
            ).start()

    everyone = sorted(
        [p for p in itertools.product(range(4), range(2), range(4), range(8)) if any(p)],
        key=lambda p: -4 * (min(p[0], 4 - p[0]) + min(p[2], 4 - p[2]) + min(p[3], 8 - p[3])) - p[1],
    )
    for c, (part, first, count) in enumerate(BACKS):
        by_parity(functools.partial(b_wait, c))
        some = pl.ds(first, count)
        x = ret[part, some]
        corr = corr + folded(sent[part, some] * x)
        square = square + folded(x * (x + 2.0 * wave[part, some]))
        last = c == len(BACKS) - 1
        if last:
            row = jnp.zeros((1, N), F32)
            for i, value in enumerate((norm, corr, square)):
                total = jnp.sum(jnp.sum(value, axis=0, keepdims=True), axis=1, keepdims=True)
                row = jnp.where(lane == i, total, row)
            row1[...] = row
            tell(everyone[:TOLD])
        x = [ret[part, first + z] for z in range(count)]
        guest = times_right(jnp.concatenate([jnp.where(holds, 0.0, a[:FOLD]) for a in x], axis=0), gi[...])
        live = [b for a in x for b in (jnp.where(holds, a[:FOLD], 0.0), a[FOLD:])]
        live = times_right(jnp.concatenate(live, axis=0), ri[...])
        x = [
            jnp.concatenate([live[z * LIVE : (z + 1) * LIVE], guest[z * FOLD : (z + 1) * FOLD]], axis=0)
            for z in range(count)
        ]
        x = times_left(li[...], jnp.concatenate(x, axis=1))
        for z in range(count):
            app[part, first + z] = x[:, z * N : (z + 1) * N] + pot[first + z] * planes[part, first + z]
        for j in y_peers:
            pltpu.make_async_remote_copy(
                app.at[part, some, pl.ds(pl.multiple_of(j * YL, YL), YL), :], out.at[part, my, some],
                o_send.at[c], o_recv.at[c],
                device_id=(j, mz), device_id_type=MESH,
            ).start()
        if last:
            tell(everyone[TOLD:])
            pltpu.make_async_copy(row1, sums.at[mine_row, :], r_own).start()
        out[part, my, some] = app[part, some, mine, :]

    for part in range(2):
        by_parity(lambda odd, part=part: drain(slot_rows(part, odd), z_send.at[part]))
    for c, (part, first, count) in enumerate(BACKS):
        by_parity(lambda odd, c=c, part=part, count=count: drain(z_rows(part, odd, count), b_send.at[c]))
        drain(app.at[part, pl.ds(first, count), others, :], o_send.at[c], f"s{c}")
        drain(out.at[part, pl.ds(0, NY - 1), pl.ds(first, count)], o_recv.at[c], f"o{c}")
    drain(pot.at[:, others, :], y_send.at[len(CHUNKS)])
    for c, (part, z, nz) in enumerate(CHUNKS):
        drain(planes.at[part, pl.ds(z, nz), others, :], y_send.at[c])

    told = sums.at[pl.ds(0, NY * NZ - 1), :]
    drain(told, r_send.at[0])
    pltpu.make_async_copy(row1, sums.at[mine_row, :], r_own).wait()
    band = lax.broadcasted_iota(jnp.int32, (NB, NB), 0)
    keep = jnp.zeros((NB, NB), F32)
    for b in range(NB):
        keep = jnp.where(band == b, 1.0 - locked[b].astype(F32), keep)
    keep_ref[...] = keep
    drain(told, r_recv.at[0], "r0")


def write_out(applied, sums, keep, out, ray_hbm, res_hbm, ray, res, sem):
    first = pltpu.make_async_copy(applied, out, sem.at[0])
    first.start()
    same = lax.broadcasted_iota(jnp.int32, (NB, NB), 0) == lax.broadcasted_iota(jnp.int32, (NB, NB), 1)
    total = jnp.sum(sums[...].reshape(NZ, NY, N), axis=0)
    norm, corr, square = (jnp.broadcast_to(total[:, i : i + 1], (NB, NB)) for i in range(3))
    rayleigh = corr / norm
    residual = jnp.sqrt((square - rayleigh * corr) / norm) * keep[...]
    ray[...] = jnp.sum(jnp.where(same, rayleigh, 0.0), axis=0)
    res[...] = jnp.sum(jnp.where(same, residual, 0.0), axis=0)
    copies = [pltpu.make_async_copy(ray, ray_hbm, sem.at[1]), pltpu.make_async_copy(res, res_hbm, sem.at[2])]
    for copy in copies:
        copy.start()
    for copy in [first, *copies]:
        copy.wait()


def body(wavefunctions, potential, cutoff_sq, locked_mask):
    consts = [jnp.asarray(t) for t in tables()]
    hbm = pl.BlockSpec(memory_space=pltpu.HBM)
    vmem = pl.BlockSpec(memory_space=pltpu.VMEM)
    dma = pltpu.SemaphoreType.DMA
    results = pl.pallas_call(
        kernel,
        out_shape=(
            pltpu.VMEM((2, NB, ZL, YL, N), F32),
            pltpu.VMEM((NZ * NY, N), F32),
            pltpu.VMEM((NB, NB), F32),
        ),
        in_specs=[hbm] * 12,
        out_specs=(vmem, vmem, vmem),
        scratch_shapes=[
            pltpu.VMEM((2, NB, ZL, YL, N), F32),
            pltpu.VMEM((ZL, YL, N), F32),
            pltpu.SMEM((1,), jnp.int32),
            pltpu.SMEM((NB,), jnp.int32),
            *[pltpu.VMEM(t.shape, BF16) for t in consts],
            pltpu.VMEM((2, ZL, N, N), F32),
            pltpu.VMEM((ZL, N, N), F32),
            pltpu.VMEM((2, ZL, LIVE, N), F32),
            pltpu.VMEM((2, NZ * ZL * SL, N), F32),
            pltpu.VMEM((2, NZ * ZL * SL, N), F32),
            pltpu.VMEM((2, ZL, LIVE, N), F32),
            pltpu.VMEM((2, ZL, LIVE, N), F32),
            pltpu.VMEM((2, ZL, N, N), F32),
            pltpu.VMEM((2, N, SL * N), F32),
            pltpu.VMEM((1, N), F32),
            dma((12,)),
            dma((len(CHUNKS) + 1,)), dma((len(CHUNKS) + 1,)), dma((2,)), dma((2,)), dma((len(BACKS),)), dma((len(BACKS),)),
            dma((len(BACKS),)), dma((len(BACKS),)), dma((len(CHUNKS) + len(BACKS),)), dma((1,)), dma((1,)), dma(()),
            pltpu.SemaphoreType.REGULAR((len(ROUNDS),)),
        ],
        compiler_params=pltpu.CompilerParams(collective_id=0, has_side_effects=True),
    )(wavefunctions, potential, cutoff_sq, locked_mask, *consts)
    return pl.pallas_call(
        write_out,
        out_shape=(
            jax.ShapeDtypeStruct((2, NB, ZL, YL, N), F32),
            jax.ShapeDtypeStruct((NB,), F32),
            jax.ShapeDtypeStruct((NB,), F32),
        ),
        in_specs=[vmem] * 3,
        out_specs=(hbm,) * 3,
        scratch_shapes=[pltpu.VMEM((NB,), F32), pltpu.VMEM((NB,), F32), dma((3,))],
    )(*[pltpu.with_memory_space_constraint(a, pltpu.VMEM) for a in results])


def solution(mesh):
    placed = (P(None, None, "pz", "py", None), P("pz", "py", None), P(), P())
    return jax.shard_map(
        body,
        mesh=mesh,
        in_specs=placed,
        out_specs=(P(None, None, "pz", "py", None), P(), P()),
        check_vma=False,
    )
```

```python
import functools
import itertools
import math

import jax
import jax.numpy as jnp
import numpy as np
from jax import lax
from jax.experimental import pallas as pl
from jax.experimental.pallas import tpu as pltpu
from jax.sharding import PartitionSpec as P

N = 128
NB = 8
NY = 8
NZ = 32
ZL = N // NZ
YL = N // NY
ENTRY = ((0, 2), (0, 6), (2, 0), (1, 1), (1, 7), (3, 1), (3, 7), (1, 0), (3, 0), (0, 1), (0, 7))
ROUNDS = (((0, 2), (0, 6), (2, 0)), ((0, 2), (0, 6)))
SENT_IN = ((0, 1, 2, 3), (), ())
BACKS = ((0, 0, 4), (1, 0, 4))
TOLD = 64
SL = N // NZ
CHUNKS = ((0, 0, 1), (0, 1, 1), (0, 2, 2), (1, 0, 4))
LIVE = 112
FOLD = N - LIVE
HOST = 48
SPHERE = N * N // 4
MESH = pl.DeviceIdType.MESH
F32 = jnp.float32
BF16 = jnp.bfloat16


def basis():
    n = np.arange(N)
    rows = []
    for m in range(N):
        k = (m + 1) // 2
        angle = 2.0 * np.pi * ((k * n) % N) / N
        row = np.cos(angle) if (m % 2 == 1 or m == 0) else np.sin(angle)
        scale = 1.0 / N if k in (0, N // 2) else 2.0 / N
        rows.append(np.sqrt(scale) * row)
    return np.stack(rows)


def high_low(table):
    high = table.astype(BF16)
    low = (table - high.astype(np.float64)).astype(BF16)
    return high, low


def row_order():
    hosts = [2 * k - 1 + c for k in range(HOST, HOST + FOLD // 2) for c in range(2)]
    guests = [2 * (111 - k) - 1 + c for k in range(HOST, HOST + FOLD // 2) for c in range(2)]
    plain = [m for m in range(N) if m not in hosts and m not in guests]
    for host, guest in zip(hosts, guests, strict=True):
        width = [sum(((m + 1) // 2) ** 2 + ((r + 1) // 2) ** 2 <= SPHERE for m in range(N)) for r in (host, guest)]
        assert sum(width) <= N
    return hosts + plain + guests


def tables():
    f = basis()
    fh, fl = high_low(f)
    ph, pl_ = fh[row_order()], fl[row_order()]
    right_fwd = np.block([[fh.T, fl.T], [fh.T, fl.T]])
    right_inv = np.block([[fh, fl], [fh, fl]])
    guest_fwd = np.block([[fh[::-1].T, fl[::-1].T], [fh[::-1].T, fl[::-1].T]])
    guest_inv = np.block([[fh[::-1], fl[::-1]], [fh[::-1], fl[::-1]]])
    left_fwd = np.block([[ph, ph], [pl_, pl_]])
    left_inv = np.block([[ph.T, ph.T], [pl_.T, pl_.T]])
    zh, zl = (t.reshape(N, NZ, ZL).swapaxes(1, 2).reshape(N, N) for t in (fh, fl))
    z_fwd = np.block([[zh, zh], [zl, zl]])
    z_inv = np.block([[zh.T, zh.T], [zl.T, zl.T]])
    return [right_fwd, guest_fwd, left_fwd, right_inv, guest_inv, left_inv, z_fwd, z_inv]


def split(x):
    high = x.astype(BF16)
    low = (x - high.astype(F32)).astype(BF16)
    return high, low


def dot(a, b):
    return jnp.dot(a, b, preferred_element_type=F32)


def times_right(x, table):
    high, low = split(x)
    both = dot(jnp.concatenate([high, low], axis=1), table)
    return both[:, :N] + both[:, N:]


def times_left(table, x):
    high, low = split(x)
    both = dot(table, jnp.concatenate([high, low], axis=0))
    return both[:N] + both[N:]


def kernel(
    u_hbm, v_hbm, cutoff_hbm, locked_hbm, rf_hbm, gf_hbm, lf_hbm, ri_hbm, gi_hbm, li_hbm, zf_hbm, zi_hbm,
    out, sums, keep_ref,
    u_in, v_in, cutoff, locked, rf, gf, lf, ri, gi, li, zf, zi,
    planes, pot, sent, got, back, ret, wave, app, kin, row1,
    in_sem, y_send, y_recv, z_send, z_recv, b_send, b_recv, o_send, o_recv, own, r_send, r_recv, r_own, rounds,
):
    my = lax.axis_index("py")
    mz = lax.axis_index("pz")

    y_chip = [lax.rem(my // 2 + d, 4) * 2 for d in range(4)]
    y_core = [lax.rem(my + d, 2) for d in range(2)]
    y_peers = [y_chip[d] + y_core[c] for d in (2, 1, 3, 0) for c in (0, 1) if d or c]
    z_x = [lax.rem(mz // 8 + d, 4) * 8 for d in range(4)]
    z_z = [lax.rem(mz + d, 8) for d in range(8)]
    by_hops = sorted(
        [p for p in itertools.product((2, 1, 3, 0), (4, 3, 5, 2, 6, 1, 7, 0)) if any(p)],
        key=lambda p: -min(p[0], 4 - p[0]) - min(p[1], 8 - p[1]),
    )
    z_peers = [(z_x[d] + z_z[e], e % 2) for d, e in by_hops]

    def load(i, source, target):
        copy = pltpu.make_async_copy(source, target, in_sem.at[i])
        copy.start()
        return copy

    first = [load(0, u_hbm, u_in), load(1, v_hbm, v_in)]
    barrier = pltpu.get_barrier_semaphore()

    def greet(sem, offsets):
        for d, e in offsets:
            pl.semaphore_signal(sem, inc=1, device_id=(my, z_x[d] + z_z[e]), device_id_type=MESH)

    greet(barrier, ENTRY)
    for j in y_peers:
        pl.semaphore_signal(barrier, inc=1, device_id=(j, mz), device_id_type=MESH)

    later = [(lf_hbm, lf), (rf_hbm, rf), (gf_hbm, gf), (cutoff_hbm, cutoff), (locked_hbm, locked), (zf_hbm, zf), (zi_hbm, zi), (ri_hbm, ri), (gi_hbm, gi), (li_hbm, li)]
    later = [load(i + 2, a, b) for i, (a, b) in enumerate(later)]
    for copy in first:
        copy.wait()
    with jax.named_scope("barrier"):
        pl.semaphore_wait(barrier, len(ENTRY) + NY - 1)

    def drain(ref, sem, name="end"):
        with jax.named_scope(name):
            pltpu.make_async_copy(ref, ref, sem).wait()

    mine = pl.ds(pl.multiple_of(my * YL, YL), YL)
    def y_out(c):
        part, z, nz = CHUNKS[c]
        for j in y_peers:
            pltpu.make_async_remote_copy(
                u_in.at[part, j, pl.ds(z, nz)], planes.at[part, pl.ds(z, nz), mine, :], y_send.at[c], y_recv.at[c],
                device_id=(j, mz), device_id_type=MESH,
            ).start()

    for r, offsets in enumerate(ROUNDS):
        if r:
            with jax.named_scope(f"round{r}"):
                pl.semaphore_wait(rounds.at[r - 1], len(ROUNDS[r - 1]))
        greet(rounds.at[r], offsets)
        for c in SENT_IN[r]:
            y_out(c)
        if r == 0:
            for j in y_peers:
                pltpu.make_async_remote_copy(
                    v_in, pot.at[:, mine, :], y_send.at[len(CHUNKS)], y_recv.at[len(CHUNKS)],
                    device_id=(j, mz), device_id_type=MESH,
                ).start()
    with jax.named_scope("roundlast"):
        pl.semaphore_wait(rounds.at[len(ROUNDS) - 1], len(ROUNDS[-1]))
    for c in SENT_IN[len(ROUNDS)]:
        y_out(c)
    planes[:, :, mine, :] = u_in[:, my]
    pot[:, mine, :] = v_in[...]
    for copy in later:
        copy.wait()

    def first_slot(d, odd, part):
        return 7 * (d // 2) + (4 - part) * odd

    def slots(odd, part):
        return 4 - (odd + part) % 2

    lane = lax.broadcasted_iota(jnp.int32, (1, N), 1)
    mine_row = pl.ds(mz * NY + my, 1)
    up = (lane + 1) // 2
    down = (N - lane) // 2
    others = pl.ds(0, (NY - 1) * YL)
    own_row = HOST + lax.broadcasted_iota(jnp.int32, (FOLD, N), 0) // 2
    own_kx = (lax.broadcasted_iota(jnp.int32, (FOLD, N), 1) + 1) // 2
    holds = own_row * own_row + own_kx * own_kx <= SPHERE

    def plane_transform(field, target, part, first, count):
        x = times_left(lf[...], jnp.concatenate([field[z] for z in range(count)], axis=1))
        x = [x[:, z * N : (z + 1) * N] for z in range(count)]
        guest = times_right(jnp.concatenate([a[LIVE:] for a in x], axis=0), gf[...])
        live = times_right(jnp.concatenate([a[:LIVE] for a in x], axis=0), rf[...])
        for z in range(count):
            a = live[z * LIVE : (z + 1) * LIVE]
            target[part, first + z, :FOLD, :] = jnp.where(holds, a[:FOLD], guest[z * FOLD : (z + 1) * FOLD])
            target[part, first + z, FOLD:, :] = a[FOLD:]

    def by_parity(act):
        for odd in range(2):
            pl.when(lax.rem(mz, 2) == odd)(functools.partial(act, odd))

    got_view = got.reshape(2, NZ, ZL, SL, N)
    back_view = back.reshape(2, NZ, ZL, SL, N)

    def z_out(part, first, count, c, odd):
        def copy_of(d, o):
            n = slots(o, part)
            return (
                sent.at[part, pl.ds(first, count), pl.ds(first_slot(d, o, part), n), :],
                got_view.at[part, mz, pl.ds(first, count), pl.ds(0, n), :],
            )

        for d, e in z_peers:
            a, b = copy_of(d, (odd + e) % 2)
            pltpu.make_async_remote_copy(
                a, b, z_send.at[part], z_recv.at[part], device_id=(my, d), device_id_type=MESH
            ).start()
        pltpu.make_async_copy(*copy_of(mz, odd), own.at[c]).start()

    def z_back(c, odd):
        part, first, count = BACKS[c]
        n = slots(odd, part)
        target = ret.at[part, pl.ds(first, count), pl.ds(first_slot(mz, odd, part), n), :]
        for d, _ in z_peers:
            pltpu.make_async_remote_copy(
                back_view.at[part, d, pl.ds(first, count), pl.ds(0, n), :], target, b_send.at[c], b_recv.at[c],
                device_id=(my, d), device_id_type=MESH,
            ).start()
        pltpu.make_async_copy(
            back_view.at[part, mz, pl.ds(first, count), pl.ds(0, n), :], target, own.at[len(CHUNKS) + c]
        ).start()

    def z_rows(part, odd, count=ZL):
        return got_view.at[part, pl.ds(0, NZ - 1), pl.ds(0, count), pl.ds(0, slots(odd, part)), :]

    def slot_rows(part, odd, count=ZL):
        return ret.at[part, pl.ds(0, count), pl.ds(0, LIVE - slots(odd, part)), :]

    def own_wait(part, count, c, odd):
        a = ret.at[part, pl.ds(0, count), pl.ds(0, slots(odd, part)), :]
        pltpu.make_async_copy(a, a, own.at[c]).wait()

    def z_wait(part, odd):
        drain(z_rows(part, odd), z_recv.at[part], f"z{part}")
        for c, (p, _, count) in enumerate(CHUNKS):
            if p == part:
                own_wait(part, count, c, odd)

    def b_wait(c, odd):
        part, _, count = BACKS[c]
        drain(slot_rows(part, odd, count), b_recv.at[c], f"b{c}")
        own_wait(part, count, len(CHUNKS) + c, odd)

    for c, (part, z, nz) in enumerate(CHUNKS):
        drain(planes.at[part, pl.ds(z, nz), others, :], y_recv.at[c], f"y{c}")
        plane_transform(planes[part, z : z + nz], sent, part, z, nz)
        by_parity(functools.partial(z_out, part, z, nz, c))

    for part in range(2):
        start = first_slot(mz, lax.rem(mz, 2), part)
        for i in range(SL):
            slot = start + i
            host = slot < FOLD
            ky = jnp.where(host, HOST + slot // 2, jnp.where(slot == LIVE - 1, N // 2, (slot - FOLD + 1) // 2))
            s = ky * ky + up * up
            s = jnp.where(s > jnp.where(host, SPHERE, 4 * SPHERE), (111 - ky) * (111 - ky) + down * down, s)
            kz = (lax.broadcasted_iota(jnp.int32, (N, N), 0) + 1) // 2
            s = s + kz * kz
            kin[part, :, i * N : (i + 1) * N] = jnp.where(
                s <= cutoff[0], 0.5 * (math.pi / N) ** 2 * s.astype(F32), 0.0
            )

    def folded(x):
        return jnp.sum(x.reshape(-1, 8, N), axis=0)

    drain(pot.at[:, others, :], y_recv.at[len(CHUNKS)], "pot")
    norm = corr = square = jnp.zeros((8, N), F32)
    for part in range(2):
        field = planes[part]
        local = pot[...] * field
        norm = norm + folded(field * field)
        corr = corr + folded(field * local)
        square = square + folded(local * local)
        plane_transform(local, wave, part, 0, ZL)

    for part in range(2):
        by_parity(functools.partial(z_wait, part))
        x = [
            jnp.concatenate([got[part, pl.ds(SL * z + i, NZ, stride=SL * ZL), :] for z in range(ZL)], axis=0)
            for i in range(SL)
        ]
        x = times_left(zf[...], jnp.concatenate(x, axis=1)) * kin[part]
        x = times_left(zi[...], x)
        for z in range(ZL):
            for i in range(SL):
                back[part, pl.ds(SL * z + i, NZ, stride=SL * ZL), :] = x[z * NZ : (z + 1) * NZ, i * N : (i + 1) * N]
        for c, back_chunk in enumerate(BACKS):
            if back_chunk[0] == part:
                by_parity(functools.partial(z_back, c))

    def with_total(row, i, value):
        total = jnp.sum(jnp.sum(value, axis=0, keepdims=True), axis=1, keepdims=True)
        return jnp.where(lane == i, total, row)

    row1[...] = with_total(jnp.zeros((1, N), F32), 0, norm)

    def tell(offsets):
        for a, b, d, e in offsets:
            pltpu.make_async_remote_copy(
                row1, sums.at[mine_row, :], r_send.at[0], r_recv.at[0],
                device_id=(y_chip[a] + y_core[b], z_x[d] + z_z[e]), device_id_type=MESH,
            ).start()

    everyone = sorted(
        [p for p in itertools.product(range(4), range(2), range(4), range(8)) if any(p)],
        key=lambda p: -4 * (min(p[0], 4 - p[0]) + min(p[2], 4 - p[2]) + min(p[3], 8 - p[3])) - p[1],
    )
    for c, (part, first, count) in enumerate(BACKS):
        by_parity(functools.partial(b_wait, c))
        some = pl.ds(first, count)
        x = ret[part, some]
        corr = corr + folded(sent[part, some] * x)
        square = square + folded(x * (x + 2.0 * wave[part, some]))
        last = c == len(BACKS) - 1
        if last:
            row1[...] = with_total(with_total(row1[...], 1, corr), 2, square)
            tell(everyone[:TOLD])
        x = [ret[part, first + z] for z in range(count)]
        guest = times_right(jnp.concatenate([jnp.where(holds, 0.0, a[:FOLD]) for a in x], axis=0), gi[...])
        live = [b for a in x for b in (jnp.where(holds, a[:FOLD], 0.0), a[FOLD:])]
        live = times_right(jnp.concatenate(live, axis=0), ri[...])
        x = [
            jnp.concatenate([live[z * LIVE : (z + 1) * LIVE], guest[z * FOLD : (z + 1) * FOLD]], axis=0)
            for z in range(count)
        ]
        x = times_left(li[...], jnp.concatenate(x, axis=1))
        for z in range(count):
            app[part, first + z] = x[:, z * N : (z + 1) * N] + pot[first + z] * planes[part, first + z]
        for j in y_peers:
            pltpu.make_async_remote_copy(
                app.at[part, some, pl.ds(pl.multiple_of(j * YL, YL), YL), :], out.at[part, my, some],
                o_send.at[c], o_recv.at[c],
                device_id=(j, mz), device_id_type=MESH,
            ).start()
        if last:
            tell(everyone[TOLD:])
            pltpu.make_async_copy(row1, sums.at[mine_row, :], r_own).start()
        out[part, my, some] = app[part, some, mine, :]

    for part in range(2):
        by_parity(lambda odd, part=part: drain(slot_rows(part, odd), z_send.at[part]))
    for c, (part, first, count) in enumerate(BACKS):
        by_parity(lambda odd, c=c, part=part, count=count: drain(z_rows(part, odd, count), b_send.at[c]))
        drain(app.at[part, pl.ds(first, count), others, :], o_send.at[c], f"s{c}")
        drain(out.at[part, pl.ds(0, NY - 1), pl.ds(first, count)], o_recv.at[c], f"o{c}")
    drain(pot.at[:, others, :], y_send.at[len(CHUNKS)])
    for c, (part, z, nz) in enumerate(CHUNKS):
        drain(planes.at[part, pl.ds(z, nz), others, :], y_send.at[c])

    told = sums.at[pl.ds(0, NY * NZ - 1), :]
    drain(told, r_send.at[0])
    pltpu.make_async_copy(row1, sums.at[mine_row, :], r_own).wait()
    band = lax.broadcasted_iota(jnp.int32, (NB, NB), 0)
    keep = jnp.zeros((NB, NB), F32)
    for b in range(NB):
        keep = jnp.where(band == b, 1.0 - locked[b].astype(F32), keep)
    keep_ref[...] = keep
    drain(told, r_recv.at[0], "r0")


def write_out(applied, sums, keep, out, ray_hbm, res_hbm, ray, res, sem):
    first = pltpu.make_async_copy(applied, out, sem.at[0])
    first.start()
    same = lax.broadcasted_iota(jnp.int32, (NB, NB), 0) == lax.broadcasted_iota(jnp.int32, (NB, NB), 1)
    total = jnp.sum(sums[...].reshape(NZ, NY, N), axis=0)
    norm, corr, square = (jnp.broadcast_to(total[:, i : i + 1], (NB, NB)) for i in range(3))
    rayleigh = corr / norm
    residual = jnp.sqrt((square - rayleigh * corr) / norm) * keep[...]
    ray[...] = jnp.sum(jnp.where(same, rayleigh, 0.0), axis=0)
    res[...] = jnp.sum(jnp.where(same, residual, 0.0), axis=0)
    copies = [pltpu.make_async_copy(ray, ray_hbm, sem.at[1]), pltpu.make_async_copy(res, res_hbm, sem.at[2])]
    for copy in copies:
        copy.start()
    for copy in [first, *copies]:
        copy.wait()


def body(wavefunctions, potential, cutoff_sq, locked_mask):
    consts = [jnp.asarray(t) for t in tables()]
    hbm = pl.BlockSpec(memory_space=pltpu.HBM)
    vmem = pl.BlockSpec(memory_space=pltpu.VMEM)
    dma = pltpu.SemaphoreType.DMA
    results = pl.pallas_call(
        kernel,
        out_shape=(
            pltpu.VMEM((2, NB, ZL, YL, N), F32),
            pltpu.VMEM((NZ * NY, N), F32),
            pltpu.VMEM((NB, NB), F32),
        ),
        in_specs=[hbm] * 12,
        out_specs=(vmem, vmem, vmem),
        scratch_shapes=[
            pltpu.VMEM((2, NB, ZL, YL, N), F32),
            pltpu.VMEM((ZL, YL, N), F32),
            pltpu.SMEM((1,), jnp.int32),
            pltpu.SMEM((NB,), jnp.int32),
            *[pltpu.VMEM(t.shape, BF16) for t in consts],
            pltpu.VMEM((2, ZL, N, N), F32),
            pltpu.VMEM((ZL, N, N), F32),
            pltpu.VMEM((2, ZL, LIVE, N), F32),
            pltpu.VMEM((2, NZ * ZL * SL, N), F32),
            pltpu.VMEM((2, NZ * ZL * SL, N), F32),
            pltpu.VMEM((2, ZL, LIVE, N), F32),
            pltpu.VMEM((2, ZL, LIVE, N), F32),
            pltpu.VMEM((2, ZL, N, N), F32),
            pltpu.VMEM((2, N, SL * N), F32),
            pltpu.VMEM((1, N), F32),
            dma((12,)),
            dma((len(CHUNKS) + 1,)), dma((len(CHUNKS) + 1,)), dma((2,)), dma((2,)), dma((len(BACKS),)), dma((len(BACKS),)),
            dma((len(BACKS),)), dma((len(BACKS),)), dma((len(CHUNKS) + len(BACKS),)), dma((1,)), dma((1,)), dma(()),
            pltpu.SemaphoreType.REGULAR((len(ROUNDS),)),
        ],
        compiler_params=pltpu.CompilerParams(collective_id=0, has_side_effects=True),
    )(wavefunctions, potential, cutoff_sq, locked_mask, *consts)
    return pl.pallas_call(
        write_out,
        out_shape=(
            jax.ShapeDtypeStruct((2, NB, ZL, YL, N), F32),
            jax.ShapeDtypeStruct((NB,), F32),
            jax.ShapeDtypeStruct((NB,), F32),
        ),
        in_specs=[vmem] * 3,
        out_specs=(hbm,) * 3,
        scratch_shapes=[pltpu.VMEM((NB,), F32), pltpu.VMEM((NB,), F32), dma((3,))],
    )(*[pltpu.with_memory_space_constraint(a, pltpu.VMEM) for a in results])


def solution(mesh):
    placed = (P(None, None, "pz", "py", None), P("pz", "py", None), P(), P())
    return jax.shard_map(
        body,
        mesh=mesh,
        in_specs=placed,
        out_specs=(P(None, None, "pz", "py", None), P(), P()),
        check_vma=False,
    )
```
